32 devices in a mesh: depth: 8 (over z, x), tile: 4 (over y, core).
Axes of the slice: x: 2, y: 2, z: 4, core: 2. Of those that a mesh axis runs over, the one named last changes fastest.
Arguments:
- volume: bfloat16 [64, 256, 4096], P('depth', 'tile'), may hold values from -6 to 6
- shear: int32 [64], replicated, may hold values from -64 to 64, as said below
- footprint: int32 [8, 2], P('depth'), may hold values from 0 to 4096, as said below
Outputs:
- frame: float32 [4, 256, 4096], P(None, 'tile', 'depth')
The draws below stay inside these ranges and needn't reach their ends.
Inputs may be any that keep to these rules, and one draw needn't show every extreme that they name: Offsets follow a linear tilt over the slices with small jitter; shear[0] and shear[63] are the two ends of the range, in either order. footprint[b, 0] < 1024 and footprint[b, 1] > 3072 for every brick.
All inputs are finite; a program needn't handle non-finite values.
Results may differ from the reference program's by a relative error of at most 0.00085.
Values may be sent and summed in bfloat16 or wider, within the bound.
No kernel may reach another device: no remote copies, remote signals or barrier semaphores. Data moves between devices by JAX's collectives and lax.ppermute only.
A program may use at most 64 MiB of HBM per device.

```python
import jax
import jax.numpy as jnp
from jax import lax

NY = 4096
DZ = 8
SMAX = 64
BRICKS = 8
NZ = 64
NX = 256


def draw_shear(key, part):
    first, second = jax.random.split(jax.random.fold_in(key, 11))
    sign = jax.random.randint(first, (), 0, 2) * 2 - 1
    slices = jnp.arange(NZ, dtype=jnp.int32)
    base = (2 * slices - NZ) * SMAX // NZ * sign
    jitter = jax.random.randint(second, (NZ,), -2, 3)
    offsets = jnp.clip(base + jitter, -SMAX, SMAX)
    offsets = offsets.at[0].set(-SMAX * sign).at[NZ - 1].set(SMAX * sign)
    return offsets.astype(jnp.int32)


def draw_footprint(key, part):
    first, second = jax.random.split(jax.random.fold_in(key, 23))
    count = NZ // DZ
    low = jax.random.randint(first, (count,), 0, NY // 4)
    high = NY - jax.random.randint(second, (count,), 0, NY // 4)
    low = low.at[0].set(0)
    high = high.at[count - 1].set(NY)
    return jnp.stack([low, high], axis=1).astype(jnp.int32)


def steps_of(rng, dims, cuts, least, high):
    def one(position, blocks):
        steps = jax.random.uniform(jax.random.fold_in(jax.random.fold_in(rng, 6), position), (blocks,), jnp.float32, least / len(cuts), high / len(cuts))
        return jnp.repeat(jnp.exp(steps), dims[position] // blocks).reshape((-1,) + (1,) * (len(dims) - position - 1))

    loudness = one(*cuts[0])
    for cut in cuts[1:]:
        loudness = loudness * one(*cut)
    return loudness


def bell_draw(rng, extent, spread, limit, shards=(), kind=jnp.bfloat16):
    result = spread * jax.random.normal(rng, extent, jnp.float32)
    if shards:
        result = result * steps_of(rng, extent, shards, -0.22, 0.18)
    return jnp.clip(result, -limit, limit).astype(kind)


def setup_inputs(seed: int = 0) -> dict:
    key_list = jax.random.split(jax.random.key(seed), 4)
    return {
        "volume": bell_draw(key_list[0], (NZ, NX, NY), 1.0, 6.0, ((0, 8), (1, 4))),
        "shear": draw_shear(jax.random.fold_in(key_list[3], 71), 0),
        "footprint": draw_footprint(jax.random.fold_in(key_list[3], 71), 0),
    }


def colour(cur, gx, gy, gz, offset, low, high, absorb):
    norm = jnp.sqrt(gx * gx + gy * gy + gz * gz + 1.0)
    shade = 0.3 + 0.7 * jnp.abs(0.48 * gx + 0.6 * gy + 0.64 * gz) / norm
    alpha = 1.0 - jnp.exp(-absorb * cur * cur)
    rgba = jnp.stack([shade * jax.nn.sigmoid(1.2 * cur + 0.2) * alpha, shade * jax.nn.sigmoid(-0.8 * cur) * alpha, shade * jax.nn.sigmoid(0.5 * cur - 0.3) * alpha, alpha])
    padded = jnp.pad(rgba, ((0, 0), (0, 0), (SMAX, SMAX)))
    moved = lax.dynamic_slice_in_dim(padded, (SMAX - offset).astype(jnp.int32), NY, 2)
    column = jnp.arange(NY, dtype=jnp.int32)
    inside = ((column >= low) & (column < high)).astype(jnp.float32)
    return moved * inside

def reference(volume, shear, footprint):
    flip = shear[0] > shear[NZ - 1]
    ascending = jnp.arange(BRICKS, dtype=jnp.int32)
    order = jnp.where(flip, BRICKS - 1 - ascending, ascending).astype(jnp.int32)
    absorb = 2.0 / NZ

    def brick_step(image, brick):

        def slice_step(acc, step):
            local = jnp.where(flip, DZ - 1 - step, step).astype(jnp.int32)
            index = (brick * DZ + local).astype(jnp.int32)
            cur = lax.dynamic_index_in_dim(volume, index, 0, keepdims=False).astype(jnp.float32)
            prev = lax.dynamic_index_in_dim(volume, jnp.maximum(index - 1, 0).astype(jnp.int32), 0, keepdims=False).astype(jnp.float32)
            nxt = lax.dynamic_index_in_dim(volume, jnp.minimum(index + 1, NZ - 1).astype(jnp.int32), 0, keepdims=False).astype(jnp.float32)
            prev = jnp.where(index > 0, prev, 0.0)
            nxt = jnp.where(index < NZ - 1, nxt, 0.0)
            gz = 0.5 * (nxt - prev)
            rows = jnp.pad(cur, ((1, 1), (0, 0)))
            gx = 0.5 * (rows[2:] - rows[:-2])
            cols = jnp.pad(cur, ((0, 0), (1, 1)))
            gy = 0.5 * (cols[:, 2:] - cols[:, :-2])
            placed = colour(cur, gx, gy, gz, shear[index], footprint[brick, 0], footprint[brick, 1], absorb)
            return (acc + (1.0 - acc[3:4]) * placed, None)
        acc, _ = lax.scan(slice_step, jnp.zeros((4, NX, NY), jnp.float32), jnp.arange(DZ, dtype=jnp.int32))
        partial_value = lax.optimization_barrier(acc.astype(jnp.bfloat16)).astype(jnp.float32)
        return (image + (1.0 - image[3:4]) * partial_value, None)
    frame, _ = lax.scan(brick_step, jnp.zeros((4, NX, NY), jnp.float32), order)
    return frame
```

```python
import functools

import jax
import jax.numpy as jnp
from jax import lax
from jax.experimental import pallas as pl
from jax.experimental.pallas import tpu as pltpu
from jax.sharding import PartitionSpec as P

SMAX = 64
LANES = 128
ROWS = 16
LOG2E = 1.4426950408889634


def neighbours(x, axis, length):
    up = [(i, i + 1) for i in range(length - 1)]
    down = [(i + 1, i) for i in range(length - 1)]
    return up, down


def partial_kernel(
    absorb, low_high, shear, vol, prev, nxt, above, below, out, field, shades
):
    slices, rows, ny = vol.shape
    width = out.shape[3]
    low, high, flip = low_high[0], low_high[1], low_high[2]
    tiles = ny // LANES
    strips = rows // ROWS

    edge = jnp.zeros((slices + 2, rows + 16, LANES), jnp.float32)
    field[:, :, 0:LANES] = edge
    field[:, :, LANES + ny : 2 * LANES + ny] = edge
    shades[:, :, 0:LANES] = jnp.zeros((slices, ROWS, LANES), jnp.float32)
    shades[:, :, LANES + ny : 2 * LANES + ny] = jnp.zeros((slices, ROWS, LANES), jnp.float32)
    top = above[...].astype(jnp.float32)
    bottom = below[...].astype(jnp.float32)
    for s in range(slices):
        field[1 + s, 7:8, LANES : LANES + ny] = top[s : s + 1]
        field[1 + s, 8 + rows : 9 + rows, LANES : LANES + ny] = bottom[s : s + 1]

    def widen(strip, carry):
        r = pl.multiple_of(strip * ROWS, ROWS)
        source = pl.ds(r, ROWS)
        target = pl.ds(pl.multiple_of(r + 8, 8), ROWS)
        for s in range(slices):
            field[1 + s, target, LANES : LANES + ny] = vol[s, source, :].astype(jnp.float32)
        field[0, target, LANES : LANES + ny] = prev[source, :].astype(jnp.float32)
        field[slices + 1, target, LANES : LANES + ny] = nxt[source, :].astype(jnp.float32)
        return carry

    lax.fori_loop(0, strips, widen, 0)

    lane = lax.broadcasted_iota(jnp.int32, (ROWS, LANES), 1)
    span = 512

    def strip_step(strip, carry):
        r = pl.multiple_of(strip * ROWS, ROWS)

        def shade_step(i, carry):
            s = i // (ny // span)
            base = pl.multiple_of((i % (ny // span)) * span, span)
            here = pl.ds(pl.multiple_of(r + 8, 8), ROWS)
            wide = pl.ds(base, span + 2 * LANES)
            mid = pl.ds(pl.multiple_of(base + LANES, LANES), span)
            line = field[s + 1, here, wide]
            dy = line[:, LANES + 1 : LANES + 1 + span] - line[:, LANES - 1 : LANES - 1 + span]
            dz = field[s + 2, here, mid] - field[s, here, mid]
            tall = field[s + 1, pl.ds(r, ROWS + 16), mid]
            dx = tall[9 : 9 + ROWS] - tall[7 : 7 + ROWS]
            squares = dx * dx + dy * dy + dz * dz + 4.0
            along = (0.7 * 0.48) * dx + (0.7 * 0.6) * dy + (0.7 * 0.64) * dz
            shades[s, :, mid] = 0.15 + 0.5 * jnp.abs(along) * lax.rsqrt(squares)
            return carry

        lax.fori_loop(0, slices * (ny // span), shade_step, 0)

        def column_step(pair, carry):
            rate = []
            for j in range(2):
                column = lane + (2 * pair + j) * LANES
                inside = (column >= low) & (column < high)
                rate.append(jnp.where(inside, -absorb * LOG2E, 0.0))
            zero = jnp.zeros((ROWS, LANES), jnp.float32)
            clear = [zero + 1.0] * 2
            total = [zero] * 2
            colours = [[zero] * 3 for _ in range(2)]
            for step in range(slices):
                s = jnp.where(flip > 0, slices - 1 - step, step)
                shift = shear[s]
                turn = jnp.where(shift < 0, shift + LANES, shift)
                first = 2 * pair + jnp.where(shift < 0, 1, 0)
                moved = []
                for ref, index, height in ((field, s + 1, r + 8), (shades, s, 0)):
                    rolled = []
                    for j in range(3):
                        at = pl.ds(pl.multiple_of((first + j) * LANES, LANES), LANES)
                        if ref is field:
                            block = ref[index, pl.ds(pl.multiple_of(height, 8), ROWS), at]
                        else:
                            block = ref[index, :, at]
                        rolled.append(pltpu.roll(block, turn, 1))
                    moved.append(
                        [jnp.where(lane < turn, rolled[j], rolled[j + 1]) for j in range(2)]
                    )
                for j in range(2):
                    v, half_shade = moved[0][j], moved[1][j]
                    left = clear[j] * jnp.exp2(v * v * rate[j])
                    weight = (clear[j] - left) * half_shade
                    clear[j] = left
                    total[j] = total[j] + weight
                    arguments = (0.6 * v + 0.1, -0.4 * v, 0.25 * v - 0.15)
                    for c in range(3):
                        colours[j][c] = colours[j][c] + weight * jnp.tanh(arguments[c])
            for j in range(2):
                tile = 2 * pair + j
                per = width // LANES
                owner = tile // per
                at = pl.ds(pl.multiple_of((tile % per) * LANES, LANES), LANES)
                for c in range(3):
                    out[owner, c, pl.ds(r, ROWS), at] = (total[j] + colours[j][c]).astype(out.dtype)
                out[owner, 3, pl.ds(r, ROWS), at] = (1.0 - clear[j]).astype(out.dtype)
            return carry

        lax.fori_loop(0, tiles // 2, column_step, 0)
        return carry

    lax.fori_loop(0, strips, strip_step, 0)


def frame_kernel(flags, pieces, out):
    bricks = pieces.shape[0]
    rows = pieces.shape[2]

    def strip_step(strip, carry):
        at = pl.ds(pl.multiple_of(strip * ROWS, ROWS), ROWS)
        image = [jnp.zeros((ROWS, out.shape[2]), jnp.float32) for _ in range(4)]
        for position in range(bricks):
            source = jnp.where(flags[2] > 0, bricks - 1 - position, position)
            clear = 1.0 - image[3]
            image = [
                image[c] + clear * pieces[source, c, at, :].astype(jnp.float32) for c in range(4)
            ]
        for c in range(4):
            out[c, at, :] = image[c]
        return carry

    lax.fori_loop(0, rows // ROWS, strip_step, 0)


def shards(volume, shear, footprint):
    slices, rows, ny = volume.shape
    bricks = lax.axis_size("depth")
    tiles = lax.axis_size("tile")
    total = slices * bricks
    flip = (shear[0] > shear[total - 1]).astype(jnp.int32)
    me = lax.axis_index("depth")
    local_shear = lax.dynamic_slice_in_dim(shear, me * slices, slices, 0)
    flags = jnp.stack([footprint[0, 0], footprint[0, 1], flip])
    up, down = neighbours(volume, "depth", bricks)
    row_up, row_down = neighbours(volume, "tile", tiles)
    above = lax.ppermute(volume[:, rows - 1, :], "tile", row_up)
    below = lax.ppermute(volume[:, 0, :], "tile", row_down)
    prev = lax.ppermute(volume[slices - 1], "depth", up)
    nxt = lax.ppermute(volume[0], "depth", down)
    vmem = pl.BlockSpec(memory_space=pltpu.VMEM)
    smem = pl.BlockSpec(memory_space=pltpu.SMEM)
    width = ny // bricks
    partial_value = pl.pallas_call(
        functools.partial(partial_kernel, 2.0 / total),
        out_shape=jax.ShapeDtypeStruct((bricks, 4, rows, width), jnp.bfloat16),
        in_specs=[smem, smem] + [vmem] * 5,
        out_specs=vmem,
        scratch_shapes=[
            pltpu.VMEM((slices + 2, rows + 16, ny + 2 * LANES), jnp.float32),
            pltpu.VMEM((slices, ROWS, ny + 2 * LANES), jnp.float32),
        ],
        name="partial",
    )(flags, local_shear, volume, prev, nxt, above, below)
    pieces = lax.all_to_all(partial_value, "depth", split_axis=0, concat_axis=0, tiled=True)
    return pl.pallas_call(
        frame_kernel,
        out_shape=jax.ShapeDtypeStruct((4, rows, width), jnp.float32),
        in_specs=[smem, vmem],
        out_specs=vmem,
        name="frame",
    )(flags, pieces)


def solution(mesh):
    placed = (P("depth", "tile", None), P(), P("depth", None))
    return jax.shard_map(
        shards, mesh=mesh, in_specs=placed, out_specs=P(None, "tile", "depth"), check_vma=False
    )
```

```python
import functools

import jax
import jax.numpy as jnp
from jax import lax
from jax.experimental import pallas as pl
from jax.experimental.pallas import tpu as pltpu
from jax.sharding import PartitionSpec as P

LANES = 128
ROWS = 16
LOG2E = 1.4426950408889634
LINK = jnp.int16
CHUNKS = 2


def shade_slice(field, moved_v, moved_s, where, shift, base, r):
    tiles = field.shape[1] - 2
    lane = lax.broadcasted_iota(jnp.int32, (ROWS, LANES), 1)
    leftmost, rightmost = lane == 0, lane == LANES - 1
    turn = jnp.where(shift < 0, shift + LANES, shift)
    here, up, down = pl.ds(r + 8, ROWS), pl.ds(r + 7, ROWS), pl.ds(r + 9, ROWS)
    zero = jnp.zeros((ROWS, LANES), jnp.float32)
    v = field[where, 1, here, :]
    ahead = pltpu.roll(v, LANES - 1, 1)
    behind_last = zero
    for t in range(1, tiles + 1):
        v_next = field[where, t + 1, here, :] if t < tiles else zero
        ahead_next = pltpu.roll(v_next, LANES - 1, 1) if t < tiles else zero
        behind = pltpu.roll(v, 1, 1)
        dy = jnp.where(rightmost, ahead_next, ahead) - jnp.where(leftmost, behind_last, behind)
        dz = field[where + 1, t, here, :] - field[where - 1, t, here, :]
        dx = field[where, t, down, :] - field[where, t, up, :]
        squares = (dx * dx + dy * dy) + (dz * dz + 4.0)
        along = (0.35 * 0.48) * dx + (0.35 * 0.6) * dy + (0.35 * 0.64) * dz
        half = 0.15 + jnp.abs(along) * lax.rsqrt(squares)
        moved_v[base, t] = pltpu.roll(v, turn, 1)
        moved_s[base, t] = pltpu.roll(half, turn, 1)
        v, ahead, behind_last = v_next, ahead_next, behind


def blend(state, moved_v, moved_s, index, shift, first, count, rate):
    lane = lax.broadcasted_iota(jnp.int32, (ROWS, LANES), 1)
    turn = jnp.where(shift < 0, shift + LANES, shift)
    start = first + jnp.where(shift < 0, 1, 0)
    keep = lane < turn
    values = [moved_v[index, start + j] for j in range(count + 1)]
    shades = [moved_s[index, start + j] for j in range(count + 1)]
    result = []
    for j in range(count):
        clear, total, colours = state[j]
        v = jnp.where(keep, values[j], values[j + 1])
        half = jnp.where(keep, shades[j], shades[j + 1])
        left = clear * jnp.exp2(v * v * rate[j])
        weight = (clear - left) * half
        arguments = (0.6 * v + 0.1, -0.4 * v, 0.25 * v - 0.15)
        colours = [colours[c] + weight * jnp.tanh(arguments[c]) for c in range(3)]
        result.append((left, total + weight, colours))
    return result


def rates(absorb, footprint, first, count):
    lane = lax.broadcasted_iota(jnp.int32, (ROWS, LANES), 1)
    found = []
    for j in range(count):
        column = lane + (first + j) * LANES
        inside = (column >= footprint[0, 0]) & (column < footprint[0, 1])
        found.append(jnp.where(inside, -absorb * LOG2E, 0.0))
    return found


def fresh(count):
    zero = jnp.zeros((ROWS, LANES), jnp.float32)
    return [(zero + 1.0, zero, [zero] * 3) for _ in range(count)]


def widen(field, index, source, row, r):
    line = source[pl.ds(row, ROWS), :].astype(jnp.float32)
    for t in range(field.shape[1] - 2):
        field[index, t + 1, pl.ds(r + 8, ROWS), :] = line[:, t * LANES : (t + 1) * LANES]


def clear_edges(field, moved_v, moved_s):
    tiles = field.shape[1] - 2
    zero = jnp.zeros((moved_v.shape[0], ROWS, LANES), jnp.float32)
    for t in (0, tiles + 1):
        moved_v[:, t] = zero
        moved_s[:, t] = zero


def inner_kernel(absorb, shear, footprint, vol, above, below, out, field, moved_v, moved_s):
    slices, rows, ny = vol.shape
    me = lax.axis_index("depth")
    flip = shear[0] > shear[shear.shape[0] - 1]
    tiles = ny // LANES
    strips = rows // ROWS
    clear_edges(field, moved_v, moved_s)
    top = above[...].astype(jnp.float32)
    bottom = below[...].astype(jnp.float32)
    for s in range(1, slices - 1):
        for t in range(tiles):
            at = slice(t * LANES, (t + 1) * LANES)
            field[s, t + 1, 7:8, :] = top[s : s + 1, at]
            field[s, t + 1, 8 + rows : 9 + rows, :] = bottom[s : s + 1, at]

    def widen_step(i, carry):
        s = i // strips
        r = pl.multiple_of((i % strips) * ROWS, ROWS)
        widen(field, s, vol.at[s], r, r)
        return carry

    lax.fori_loop(0, slices * strips, widen_step, 0)

    def strip_step(strip, carry):
        r = pl.multiple_of(strip * ROWS, ROWS)

        def shade_step(i, carry):
            shade_slice(field, moved_v, moved_s, i + 1, shear[me * slices + i + 1], i, r)
            return carry

        lax.fori_loop(0, slices - 2, shade_step, 0)

        def column_step(pair, carry):
            first = 2 * pair
            rate = rates(absorb, footprint, first, 2)
            state = fresh(2)
            for step in range(slices - 2):
                i = jnp.where(flip, slices - 3 - step, step)
                shift = shear[me * slices + i + 1]
                state = blend(state, moved_v, moved_s, i, shift, first, 2, rate)
            for j in range(2):
                at = pl.ds(pl.multiple_of((first + j) * LANES, LANES), LANES)
                clear, total, colours = state[j]
                for c in range(3):
                    out[c, pl.ds(r, ROWS), at] = total + colours[c]
                out[3, pl.ds(r, ROWS), at] = clear
            return carry

        lax.fori_loop(0, tiles // 2, column_step, 0)
        return carry

    lax.fori_loop(0, strips, strip_step, 0)


def outer_kernel(
    absorb, inner, row0, shear, footprint, vol, above, below, prev, nxt, mid, *rest
):
    outs, (field, moved_v, moved_s) = rest[:inner], rest[inner:]
    slices, rows, ny = vol.shape
    chunk = outs[0].shape[2]
    groups = outs[0].shape[0]
    width = outs[0].shape[3]
    me = lax.axis_index("depth")
    flip = shear[0] > shear[shear.shape[0] - 1]
    tiles = ny // LANES
    strips = chunk // ROWS
    clear_edges(field, moved_v, moved_s)
    for index, s in ((1, 0), (4, slices - 1)):
        for edge, row, place in ((above, row0 - 1, 7), (below, row0 + chunk, 8 + chunk)):
            if 0 <= row < rows:
                first = row // ROWS * ROWS
                line = vol[s, first : first + ROWS, :].astype(jnp.float32)
                line = line[row - first : row - first + 1]
            else:
                line = edge[...].astype(jnp.float32)[s : s + 1]
            for t in range(tiles):
                field[index, t + 1, place : place + 1, :] = line[:, t * LANES : (t + 1) * LANES]

    def widen_step(strip, carry):
        r = pl.multiple_of(strip * ROWS, ROWS)
        row = pl.multiple_of(row0 + r, ROWS)
        sources = (prev, vol.at[0], vol.at[1], vol.at[slices - 2], vol.at[slices - 1], nxt)
        for index, source in enumerate(sources):
            widen(field, index, source, row, r)
        return carry

    lax.fori_loop(0, strips, widen_step, 0)
    per = width // LANES
    count = min(2, per)

    def strip_step(strip, carry):
        r = pl.multiple_of(strip * ROWS, ROWS)

        def shade_step(i, carry):
            shift = shear[me * slices + i * (slices - 1)]
            shade_slice(field, moved_v, moved_s, 1 + 3 * i, shift, i, r)
            return carry

        lax.fori_loop(0, 2, shade_step, 0)
        for slot in range(inner):
            column = lax.rem(lax.rem(me, inner) + slot, inner)

            def column_step(i, carry, slot=slot, column=column):
                group, part = i // (per // count), lax.rem(i, per // count)
                first = (group * inner + column) * per + part * count
                rate = rates(absorb, footprint, first, count)
                state = fresh(count)
                for step in range(2):
                    i = jnp.where(flip, 1 - step, step)
                    shift = shear[me * slices + i * (slices - 1)]
                    state = blend(state, moved_v, moved_s, i, shift, first, count, rate)
                    if step == 0:
                        for j in range(count):
                            at = pl.ds(pl.multiple_of((first + j) * LANES, LANES), LANES)
                            row = pl.ds(pl.multiple_of(row0 + r, ROWS), ROWS)
                            clear, total, colours = state[j]
                            colours = [
                                colours[c] + clear * mid[c, row, at] for c in range(3)
                            ]
                            state[j] = (clear * mid[3, row, at], total, colours)
                for j in range(count):
                    at = pl.ds(pl.multiple_of((part * count + j) * LANES, LANES), LANES)
                    clear, total, colours = state[j]
                    for c in range(3):
                        image = total + colours[c]
                        outs[slot][group, c, pl.ds(r, ROWS), at] = image.astype(jnp.bfloat16)
                    outs[slot][group, 3, pl.ds(r, ROWS), at] = (1.0 - clear).astype(jnp.bfloat16)
                return carry

            lax.fori_loop(0, groups * (per // count), column_step, 0)
        return carry

    lax.fori_loop(0, strips, strip_step, 0)


def encode(x):
    code = (jnp.sqrt(jnp.clip(x, 0.0, 1.0)) * 65535.0 + 0.5).astype(jnp.int32) - 32768
    return code.astype(LINK)


def decode(code):
    root = (code.astype(jnp.int32) + 32768).astype(jnp.float32) * (1.0 / 65535.0)
    return root * root


def over(pieces):
    image = pieces[0]
    for piece in pieces[1:]:
        clear = 1.0 - image[3]
        image = [image[c] + clear * piece[c] for c in range(4)]
    return image


def group_kernel(inner, shear, *rest):
    sources, outs = rest[:inner], rest[inner:-1]
    held = rest[-1]
    me = lax.axis_index("depth")
    flip = shear[0] > shear[shear.shape[0] - 1]
    column, group = lax.rem(me, inner), lax.div(me, inner)
    groups, _, chunk, width = sources[0].shape
    for k in range(inner):
        held[lax.rem(column - k + inner, inner)] = sources[k][...]

    def step(i, carry):
        r = pl.multiple_of(i * ROWS, ROWS)
        for k in range(groups):
            target = lax.rem(group + k, groups)
            pieces = []
            for position in range(inner):
                x = jnp.where(flip, inner - 1 - position, position)
                pieces.append(
                    [
                        held[x, target, c, pl.ds(r, ROWS), :].astype(jnp.float32)
                        for c in range(4)
                    ]
                )
            image = over(pieces)
            for c in range(4):
                outs[k][c, pl.ds(r, ROWS), :] = encode(image[c])
        return carry

    lax.fori_loop(0, chunk // ROWS, step, 0)


def frame_kernel(inner, groups, shear, *rest):
    sources, out, held = rest[:-2], rest[-2], rest[-1]
    me = lax.axis_index("depth")
    flip = shear[0] > shear[shear.shape[0] - 1]
    group = lax.div(me, inner)
    chunk = sources[0].shape[1]
    for index, source in enumerate(sources):
        part, k = index // groups, index % groups
        held[lax.rem(group - k + groups, groups), :, part * chunk : (part + 1) * chunk, :] = source[
            ...
        ]

    def step(i, carry):
        at = pl.ds(pl.multiple_of(i * ROWS, ROWS), ROWS)
        pieces = []
        for position in range(groups):
            z = jnp.where(flip, groups - 1 - position, position)
            pieces.append([decode(held[z, c, at, :]) for c in range(4)])
        image = over(pieces)
        for c in range(4):
            out[c, at, :] = image[c]
        return carry

    lax.fori_loop(0, out.shape[1] // ROWS, step, 0)


def shards(volume, shear, footprint):
    slices, rows, ny = volume.shape
    bricks = lax.axis_size("depth")
    strips = lax.axis_size("tile")
    absorb = 2.0 / (slices * bricks)
    inner = 1
    while 4 * inner * inner <= bricks:
        inner *= 2
    groups = bricks // inner
    width = ny // bricks
    tiles = ny // LANES

    def line(length):
        return [(i, i + 1) for i in range(length - 1)], [(i + 1, i) for i in range(length - 1)]

    row_up, row_down = line(strips)
    depth_up, depth_down = line(bricks)
    above = lax.ppermute(volume[:, rows - 1, :], "tile", row_up)
    below = lax.ppermute(volume[:, 0, :], "tile", row_down)
    prev = lax.ppermute(volume[slices - 1], "depth", depth_up)
    nxt = lax.ppermute(volume[0], "depth", depth_down)

    vmem = pl.BlockSpec(memory_space=pltpu.VMEM)
    smem = pl.BlockSpec(memory_space=pltpu.SMEM)
    moved = lambda n: pltpu.VMEM((n, tiles + 2, ROWS, LANES), jnp.float32)
    mid = pl.pallas_call(
        functools.partial(inner_kernel, absorb),
        out_shape=jax.ShapeDtypeStruct((4, rows, ny), jnp.float32),
        in_specs=[smem, smem] + [vmem] * 3,
        out_specs=vmem,
        scratch_shapes=[
            pltpu.VMEM((slices, tiles + 2, rows + 16, LANES), jnp.float32),
            moved(slices - 2),
            moved(slices - 2),
        ],
        cost_estimate=pl.CostEstimate(
            flops=100 * slices * rows * ny, bytes_accessed=8 << 20, transcendentals=0
        ),
        name="inner",
    )(shear, footprint, volume, above, below)

    chunk = rows // CHUNKS
    received = []
    for part in range(CHUNKS):
        sides = pl.pallas_call(
            functools.partial(outer_kernel, absorb, inner, part * chunk),
            out_shape=[jax.ShapeDtypeStruct((groups, 4, chunk, width), jnp.bfloat16)] * inner,
            in_specs=[smem, smem] + [vmem] * 6,
            out_specs=[vmem] * inner,
            scratch_shapes=[
                pltpu.VMEM((6, tiles + 2, chunk + 16, LANES), jnp.float32),
                moved(2),
                moved(2),
            ],
            cost_estimate=pl.CostEstimate(
                flops=200 * chunk * ny, bytes_accessed=4 << 20, transcendentals=0
            ),
            name="outer",
        )(shear, footprint, volume, above, below, prev, nxt, mid)
        sides = list(sides)
        for k in range(1, inner):
            pairs = [
                (g * inner + x, g * inner + (x + k) % inner)
                for g in range(groups)
                for x in range(inner)
            ]
            sides[k] = lax.ppermute(sides[k], "depth", pairs)
        pieces = pl.pallas_call(
            functools.partial(group_kernel, inner),
            out_shape=[jax.ShapeDtypeStruct((4, chunk, width), LINK)] * groups,
            in_specs=[smem] + [vmem] * inner,
            out_specs=[vmem] * groups,
            scratch_shapes=[pltpu.VMEM((inner, groups, 4, chunk, width), jnp.bfloat16)],
            cost_estimate=pl.CostEstimate(
                flops=20 * chunk * ny, bytes_accessed=2 << 20, transcendentals=0
            ),
            name="group",
        )(shear, *sides)
        pieces = list(pieces)
        for k in range(1, groups):
            pairs = [
                (g * inner + x, (g + k) % groups * inner + x)
                for g in range(groups)
                for x in range(inner)
            ]
            pieces[k] = lax.ppermute(pieces[k], "depth", pairs)
        received += pieces
    return pl.pallas_call(
        functools.partial(frame_kernel, inner, groups),
        out_shape=jax.ShapeDtypeStruct((4, rows, width), jnp.float32),
        in_specs=[smem] + [vmem] * len(received),
        out_specs=vmem,
        scratch_shapes=[pltpu.VMEM((groups, 4, rows, width), LINK)],
        name="frame",
    )(shear, *received)


def solution(mesh):
    placed = (P("depth", "tile", None), P(), P("depth", None))
    return jax.shard_map(
        shards, mesh=mesh, in_specs=placed, out_specs=P(None, "tile", "depth"), check_vma=False
    )
```

```python
import functools

import jax
import jax.numpy as jnp
from jax import lax
from jax.experimental import pallas as pl
from jax.experimental.pallas import tpu as pltpu
from jax.sharding import PartitionSpec as P

LANES = 128
ROWS = 16
LOG2E = 1.4426950408889634
LINK = jnp.int16
PARTS = 2


def params(mib):
    return pltpu.CompilerParams(vmem_limit_bytes=mib << 20)


def shade_slice(field, moved_v, moved_s, where, shift, base, r, narrow):
    tiles = field.shape[1]
    lane = lax.broadcasted_iota(jnp.int32, (ROWS, LANES), 1)
    leftmost, rightmost = lane == 0, lane == LANES - 1
    turn = jnp.where(shift < 0, shift + LANES, shift)
    here, up, down = pl.ds(r + 8, ROWS), pl.ds(r + 7, ROWS), pl.ds(r + 9, ROWS)
    zero = jnp.zeros((ROWS, LANES), jnp.float32)
    v = field[where, 0, here, :]
    ahead = pltpu.roll(v, LANES - 1, 1)
    behind_last = zero
    for t in range(tiles):
        v_next = field[where, t + 1, here, :] if t + 1 < tiles else zero
        ahead_next = pltpu.roll(v_next, LANES - 1, 1) if t + 1 < tiles else zero
        behind = pltpu.roll(v, 1, 1)
        dy = jnp.where(rightmost, ahead_next, ahead) - jnp.where(leftmost, behind_last, behind)
        dz = field[where + 1, t, here, :] - field[where - 1, t, here, :]
        dx = field[where, t, down, :] - field[where, t, up, :]
        squares = (dx * dx + dy * dy) + (dz * dz + 4.0)
        along = (0.35 * 0.48) * dx + (0.35 * 0.6) * dy + (0.35 * 0.64) * dz
        moved_s[base, t + 1] = 0.15 + jnp.abs(along) * lax.rsqrt(squares)
        v, ahead, behind_last = v_next, ahead_next, behind

    def turn_step(once, carry):
        for t in range(tiles):
            moved_v[base, t + 1] = pltpu.roll(narrow(t), turn, 1).astype(jnp.float32)
            moved_s[base, t + 1] = pltpu.roll(moved_s[base, t + 1], turn, 1)
        return carry

    lax.fori_loop(0, 1 + jnp.minimum(turn, 0), turn_step, 0)


def blend(state, moved_v, moved_s, index, shift, first, count, rate):
    lane = lax.broadcasted_iota(jnp.int32, (ROWS, LANES), 1)
    turn = jnp.where(shift < 0, shift + LANES, shift)
    start = first + jnp.where(shift < 0, 1, 0)
    keep = lane < turn
    values = [moved_v[index, start + j] for j in range(count + 1)]
    shades = [moved_s[index, start + j] for j in range(count + 1)]
    result = []
    for j in range(count):
        clear, total, colours = state[j]
        v = jnp.where(keep, values[j], values[j + 1])
        half = jnp.where(keep, shades[j], shades[j + 1])
        left = clear * jnp.exp2(v * v * rate[j])
        weight = (clear - left) * half
        arguments = (0.6 * v + 0.1, -0.4 * v, 0.25 * v - 0.15)
        colours = [colours[c] + weight * jnp.tanh(arguments[c]) for c in range(3)]
        result.append((left, total + weight, colours))
    return result


def rates(absorb, footprint, first, count):
    lane = lax.broadcasted_iota(jnp.int32, (ROWS, LANES), 1)
    found = []
    for j in range(count):
        column = lane + (first + j) * LANES
        inside = (column >= footprint[0, 0]) & (column < footprint[0, 1])
        found.append(jnp.where(inside, -absorb * LOG2E, 0.0))
    return found


def fresh(count):
    zero = jnp.zeros((ROWS, LANES), jnp.float32)
    return [(zero + 1.0, zero, [zero] * 3) for _ in range(count)]


def widen(field, index, line, r):
    line = line.astype(jnp.float32)
    for t in range(field.shape[1]):
        field[index, t, pl.ds(r + 8, ROWS), :] = line[:, t * LANES : (t + 1) * LANES]


def set_row(field, index, place, line):
    for t in range(field.shape[1]):
        field[index, t, place : place + 1, :] = line[:, t * LANES : (t + 1) * LANES]


def clear_edges(moved_v, moved_s):
    tiles = moved_v.shape[1] - 2
    zero = jnp.zeros((moved_v.shape[0], ROWS, LANES), jnp.float32)
    for t in (0, tiles + 1):
        moved_v[:, t] = zero
        moved_s[:, t] = zero


def inner_kernel(
    absorb, shear, footprint, vol, above, below, out, field, moved_v, moved_s, held, arrived
):
    slices, rows, ny = vol.shape
    me = lax.axis_index("depth")
    flip = shear[0] > shear[shear.shape[0] - 1]
    tiles = ny // LANES
    strips = rows // ROWS
    strip = pl.program_id(0)
    r = pl.multiple_of(strip * ROWS, ROWS)

    def strip_copy(k):
        at = pl.ds(pl.multiple_of(k * ROWS, ROWS), ROWS)
        return pltpu.make_async_copy(vol.at[:, at, :], held.at[:, at, :], arrived.at[k])

    def widen_strip(k):
        at = pl.multiple_of(k * ROWS, ROWS)

        def widen_step(s, carry):
            widen(field, s, held[s, pl.ds(at, ROWS), :], at)
            return carry

        lax.fori_loop(0, slices, widen_step, 0)

    @pl.when(strip == 0)
    def _():
        for k in range(strips):
            strip_copy(k).start()
        clear_edges(moved_v, moved_s)
        top = above[...].astype(jnp.float32)
        bottom = below[...].astype(jnp.float32)
        for s in range(1, slices - 1):
            set_row(field, s, 7, top[s : s + 1])
            set_row(field, s, 8 + rows, bottom[s : s + 1])
        strip_copy(0).wait()
        widen_strip(0)

    @pl.when(strip + 1 < strips)
    def _():
        strip_copy(strip + 1).wait()
        widen_strip(strip + 1)

    def shade_step(i, carry):
        narrow = lambda t: held[i + 1, pl.ds(r, ROWS), t * LANES : (t + 1) * LANES]
        shift = shear[me * slices + i + 1]
        shade_slice(field, moved_v, moved_s, i + 1, shift, i, r, narrow)
        return carry

    lax.fori_loop(0, slices - 2, shade_step, 0)

    def column_step(pair, carry):
        first = 2 * pair
        rate = rates(absorb, footprint, first, 2)
        state = fresh(2)
        for step in range(slices - 2):
            i = jnp.where(flip, slices - 3 - step, step)
            shift = shear[me * slices + i + 1]
            state = blend(state, moved_v, moved_s, i, shift, first, 2, rate)
        for j in range(2):
            at = pl.ds(pl.multiple_of((first + j) * LANES, LANES), LANES)
            clear, total, colours = state[j]
            for c in range(3):
                out[c, :, at] = total + colours[c]
            out[3, :, at] = clear
        return carry

    lax.fori_loop(0, tiles // 2, column_step, 0)


def outer_kernel(absorb, inner, row0, rows, shear, footprint, *refs):
    front, back, front_up, front_down, back_up, back_down, above, below, prev, nxt, mid = refs[:11]
    outs, (field, moved_v, moved_s) = refs[11 : 11 + inner], refs[11 + inner :]
    slices = above.shape[0]
    groups, _, _, width = outs[0].shape
    me = lax.axis_index("depth")
    flip = shear[0] > shear[shear.shape[0] - 1]
    r = row0 + pl.program_id(0) * ROWS

    @pl.when(pl.program_id(0) == 0)
    def _():
        clear_edges(moved_v, moved_s)

    for index, up, down, s in ((1, front_up, front_down, 0), (4, back_up, back_down, slices - 1)):
        at_top, at_bottom = r == 0, r + ROWS == rows
        over_line = up[0].astype(jnp.float32)[ROWS - 1 : ROWS]
        under_line = down[0].astype(jnp.float32)[0:1]
        over_edge = above[...].astype(jnp.float32)[s : s + 1]
        under_edge = below[...].astype(jnp.float32)[s : s + 1]
        set_row(field, index, 7, jnp.where(at_top, over_edge, over_line))
        set_row(field, index, 8 + ROWS, jnp.where(at_bottom, under_edge, under_line))
    for index, line in enumerate((prev, front.at[0], front.at[1], back.at[0], back.at[1], nxt)):
        widen(field, index, line[...], 0)
    for i, ref in ((0, front.at[0]), (1, back.at[1])):
        narrow = lambda t, ref=ref: ref[:, t * LANES : (t + 1) * LANES]
        shift = shear[me * slices + i * (slices - 1)]
        shade_slice(field, moved_v, moved_s, 1 + 3 * i, shift, i, 0, narrow)
    per = width // LANES
    count = min(2, per)
    for slot in range(inner):
        column = lax.rem(lax.rem(me, inner) + slot, inner)

        def column_step(i, carry, slot=slot, column=column):
            group, part = i // (per // count), lax.rem(i, per // count)
            first = (group * inner + column) * per + part * count
            rate = rates(absorb, footprint, first, count)
            state = fresh(count)
            for step in range(2):
                i = jnp.where(flip, 1 - step, step)
                shift = shear[me * slices + i * (slices - 1)]
                state = blend(state, moved_v, moved_s, i, shift, first, count, rate)
                if step == 0:
                    for j in range(count):
                        at = pl.ds(pl.multiple_of((first + j) * LANES, LANES), LANES)
                        clear, total, colours = state[j]
                        colours = [colours[c] + clear * mid[c, :, at] for c in range(3)]
                        state[j] = (clear * mid[3, :, at], total, colours)
            for j in range(count):
                at = pl.ds(pl.multiple_of((part * count + j) * LANES, LANES), LANES)
                clear, total, colours = state[j]
                for c in range(3):
                    outs[slot][group, c, :, at] = (total + colours[c]).astype(jnp.bfloat16)
                outs[slot][group, 3, :, at] = (1.0 - clear).astype(jnp.bfloat16)
            return carry

        lax.fori_loop(0, groups * (per // count), column_step, 0)


def encode(x):
    x = jnp.maximum(x, 1e-30)
    code = (x * lax.rsqrt(x) * 65535.0 + 0.5).astype(jnp.int32) - 32768
    return code.astype(LINK)


def decode(code):
    root = (code.astype(jnp.int32) + 32768).astype(jnp.float32) * (1.0 / 65535.0)
    return root * root


def over(pieces):
    image = pieces[0]
    for piece in pieces[1:]:
        clear = 1.0 - image[3]
        image = [image[c] + clear * piece[c] for c in range(4)]
    return image


def ordered(count, mine, flip, body):
    cases = {}
    for position in range(count):
        for turned in (False, True):
            order = tuple((position - p) % count for p in range(count))
            cases.setdefault(order[::-1] if turned else order, []).append((position, turned))
    for order, where in cases.items():
        chosen = functools.reduce(
            jnp.logical_or, [(mine == position) & (flip == turned) for position, turned in where]
        )
        pl.when(chosen)(functools.partial(body, order))


def group_kernel(inner, shear, *refs):
    sources, outs = refs[:inner], refs[inner:]
    me = lax.axis_index("depth")
    flip = shear[0] > shear[shear.shape[0] - 1]
    groups = len(outs)

    def body(order):
        for k in range(groups):
            target = lax.rem(lax.div(me, inner) + k, groups)
            pieces = [
                [sources[shift][target, c].astype(jnp.float32) for c in range(4)]
                for shift in order
            ]
            for c, value in enumerate(over(pieces)):
                outs[k][c] = encode(value)

    ordered(inner, lax.rem(me, inner), flip, body)


def frame_kernel(inner, aliased, shear, *refs):
    sources, out = refs[:-1], refs[-1]
    if aliased:
        sources = sources[:-1]
    me = lax.axis_index("depth")
    flip = shear[0] > shear[shear.shape[0] - 1]

    def body(order):
        pieces = [[decode(sources[shift][c]) for c in range(4)] for shift in order]
        for c, value in enumerate(over(pieces)):
            out[c] = value

    ordered(len(sources), lax.div(me, inner), flip, body)


def shards(volume, shear, footprint):
    slices, rows, ny = volume.shape
    bricks = lax.axis_size("depth")
    crosswise = lax.axis_size("tile")
    absorb = 2.0 / (slices * bricks)
    inner = 1
    while 4 * inner * inner <= bricks:
        inner *= 2
    groups = bricks // inner
    width = ny // bricks
    tiles = ny // LANES
    strips = rows // ROWS

    def line(length):
        return [(i, i + 1) for i in range(length - 1)], [(i + 1, i) for i in range(length - 1)]

    depth_up, depth_down = line(bricks)
    row_up, row_down = line(crosswise)
    prev = lax.ppermute(volume[slices - 1], "depth", depth_up)
    nxt = lax.ppermute(volume[0], "depth", depth_down)
    above = lax.ppermute(volume[:, rows - 1, :], "tile", row_up)
    below = lax.ppermute(volume[:, 0, :], "tile", row_down)

    vmem = pl.BlockSpec(memory_space=pltpu.VMEM)
    smem = pl.BlockSpec(memory_space=pltpu.SMEM)
    anywhere = pl.BlockSpec(memory_space=pl.ANY)
    moved = lambda n: pltpu.VMEM((n, tiles + 2, ROWS, LANES), jnp.float32)
    mid = pl.pallas_call(
        functools.partial(inner_kernel, absorb),
        out_shape=jax.ShapeDtypeStruct((4, rows, ny), jnp.float32),
        grid=(strips,),
        in_specs=[smem, smem, anywhere, vmem, vmem],
        out_specs=pl.BlockSpec((4, ROWS, ny), lambda i: (0, i, 0)),
        scratch_shapes=[
            pltpu.VMEM((slices, tiles, rows + 16, LANES), jnp.float32),
            moved(slices - 2),
            moved(slices - 2),
            pltpu.VMEM((slices, rows, ny), jnp.bfloat16),
            pltpu.SemaphoreType.DMA((strips,)),
        ],
        cost_estimate=pl.CostEstimate(
            flops=100 * slices * rows * ny, bytes_accessed=8 << 20, transcendentals=0
        ),
        compiler_params=params(36),
        name="inner",
    )(shear, footprint, volume, above, below)

    chunk = rows // PARTS
    frame = None
    for part in range(PARTS):
        row0 = part * chunk
        strip0 = row0 // ROWS

        def slab(size, s, move=0, strip0=strip0):
            def index(i):
                return s, jnp.clip(strip0 + i + move, 0, strips - 1), 0

            return pl.BlockSpec((size, ROWS, ny), index)

        flat = pl.BlockSpec((ROWS, ny), lambda i, strip0=strip0: (strip0 + i, 0))
        sides = pl.pallas_call(
            functools.partial(outer_kernel, absorb, inner, row0, rows),
            out_shape=[jax.ShapeDtypeStruct((groups, 4, chunk, width), jnp.bfloat16)] * inner,
            grid=(chunk // ROWS,),
            in_specs=[
                smem,
                smem,
                slab(2, 0),
                slab(2, slices // 2 - 1),
                slab(1, 0, -1),
                slab(1, 0, 1),
                slab(1, slices - 1, -1),
                slab(1, slices - 1, 1),
                vmem,
                vmem,
                flat,
                flat,
                pl.BlockSpec((4, ROWS, ny), lambda i, strip0=strip0: (0, strip0 + i, 0)),
            ],
            out_specs=[pl.BlockSpec((groups, 4, ROWS, width), lambda i: (0, 0, i, 0))] * inner,
            scratch_shapes=[pltpu.VMEM((6, tiles, 32, LANES), jnp.float32), moved(2), moved(2)],
            cost_estimate=pl.CostEstimate(
                flops=200 * chunk * ny, bytes_accessed=4 << 20, transcendentals=0
            ),
            compiler_params=params(24),
            name="outer",
        )(shear, footprint, *[volume] * 6, above, below, prev, nxt, mid)
        sides = list(sides)
        for k in range(1, inner):
            pairs = [
                (g * inner + x, g * inner + (x + k) % inner)
                for g in range(groups)
                for x in range(inner)
            ]
            sides[k] = lax.ppermute(sides[k], "depth", pairs)
        pieces = pl.pallas_call(
            functools.partial(group_kernel, inner),
            out_shape=[jax.ShapeDtypeStruct((4, chunk, width), LINK)] * groups,
            grid=(chunk // ROWS,),
            in_specs=[smem]
            + [pl.BlockSpec((groups, 4, ROWS, width), lambda i: (0, 0, i, 0))] * inner,
            out_specs=[pl.BlockSpec((4, ROWS, width), lambda i: (0, i, 0))] * groups,
            cost_estimate=pl.CostEstimate(
                flops=20 * chunk * ny, bytes_accessed=2 << 20, transcendentals=0
            ),
            compiler_params=params(16),
            name="group",
        )(shear, *sides)
        pieces = list(pieces)
        for k in range(1, groups):
            pairs = [
                (g * inner + x, (g + k) % groups * inner + x)
                for g in range(groups)
                for x in range(inner)
            ]
            pieces[k] = lax.ppermute(pieces[k], "depth", pairs)
        frame = pl.pallas_call(
            functools.partial(frame_kernel, inner, frame is not None),
            out_shape=jax.ShapeDtypeStruct((4, rows, width), jnp.float32),
            grid=(chunk // ROWS,),
            in_specs=[smem]
            + [pl.BlockSpec((4, ROWS, width), lambda i: (0, i, 0))] * groups
            + [anywhere] * (frame is not None),
            out_specs=pl.BlockSpec((4, ROWS, width), lambda i, strip0=strip0: (0, strip0 + i, 0)),
            input_output_aliases={} if frame is None else {1 + groups: 0},
            cost_estimate=pl.CostEstimate(
                flops=20 * chunk * width, bytes_accessed=2 << 20, transcendentals=0
            ),
            compiler_params=params(16),
            name="frame",
        )(shear, *pieces, *([] if frame is None else [frame]))
    return frame


def solution(mesh):
    placed = (P("depth", "tile", None), P(), P("depth", None))
    return jax.shard_map(
        shards, mesh=mesh, in_specs=placed, out_specs=P(None, "tile", "depth"), check_vma=False
    )
```

```python
import functools

import jax
import jax.numpy as jnp
from jax import lax
from jax.experimental import pallas as pl
from jax.experimental.pallas import tpu as pltpu
from jax.sharding import PartitionSpec as P

LANES = 128
ROWS = 16
LOG2E = 1.4426950408889634
LINK = jnp.int16
INNER_MIB = 60
OUTER_MIB = 60


def params(mib):
    return pltpu.CompilerParams(vmem_limit_bytes=mib << 20)


def shade_slice(field, moved_v, moved_s, where, shift, base, r, narrow):
    tiles = field.shape[1]
    lane = lax.broadcasted_iota(jnp.int32, (ROWS, LANES), 1)
    leftmost, rightmost = lane == 0, lane == LANES - 1
    turn = jnp.where(shift < 0, shift + LANES, shift)
    here, up, down = pl.ds(r + 8, ROWS), pl.ds(r + 7, ROWS), pl.ds(r + 9, ROWS)
    zero = jnp.zeros((ROWS, LANES), jnp.float32)
    v = field[where, 0, here, :]
    ahead = pltpu.roll(v, LANES - 1, 1)
    behind_last = zero
    for t in range(tiles):
        v_next = field[where, t + 1, here, :] if t + 1 < tiles else zero
        ahead_next = pltpu.roll(v_next, LANES - 1, 1) if t + 1 < tiles else zero
        behind = pltpu.roll(v, 1, 1)
        dy = jnp.where(rightmost, ahead_next, ahead) - jnp.where(leftmost, behind_last, behind)
        dz = field[where + 1, t, here, :] - field[where - 1, t, here, :]
        dx = field[where, t, down, :] - field[where, t, up, :]
        squares = (dx * dx + dy * dy) + (dz * dz + 4.0)
        along = (0.35 * 0.48) * dx + (0.35 * 0.6) * dy + (0.35 * 0.64) * dz
        moved_s[base, t + 1] = 0.15 + jnp.abs(along) * lax.rsqrt(squares)
        v, ahead, behind_last = v_next, ahead_next, behind

    def turn_step(once, carry):
        for t in range(tiles):
            moved_v[base, t + 1] = pltpu.roll(narrow(t), turn, 1).astype(jnp.float32)
            moved_s[base, t + 1] = pltpu.roll(moved_s[base, t + 1], turn, 1)
        return carry

    lax.fori_loop(0, 1 + jnp.minimum(turn, 0), turn_step, 0)


def blend(state, moved_v, moved_s, index, shift, first, count, rate):
    lane = lax.broadcasted_iota(jnp.int32, (ROWS, LANES), 1)
    turn = jnp.where(shift < 0, shift + LANES, shift)
    start = first + jnp.where(shift < 0, 1, 0)
    keep = lane < turn
    values = [moved_v[index, start + j] for j in range(count + 1)]
    shades = [moved_s[index, start + j] for j in range(count + 1)]
    result = []
    for j in range(count):
        clear, total, colours = state[j]
        v = jnp.where(keep, values[j], values[j + 1])
        half = jnp.where(keep, shades[j], shades[j + 1])
        left = clear * jnp.exp2(v * v * rate[j])
        weight = (clear - left) * half
        arguments = (0.6 * v + 0.1, -0.4 * v, 0.25 * v - 0.15)
        colours = [colours[c] + weight * jnp.tanh(arguments[c]) for c in range(3)]
        result.append((left, total + weight, colours))
    return result


def rates(absorb, footprint, first, count):
    lane = lax.broadcasted_iota(jnp.int32, (ROWS, LANES), 1)
    found = []
    for j in range(count):
        column = lane + (first + j) * LANES
        inside = (column >= footprint[0, 0]) & (column < footprint[0, 1])
        found.append(jnp.where(inside, -absorb * LOG2E, 0.0))
    return found


def fresh(count):
    zero = jnp.zeros((ROWS, LANES), jnp.float32)
    return [(zero + 1.0, zero, [zero] * 3) for _ in range(count)]


def widen(field, index, line, place):
    line = line.astype(jnp.float32)
    for t in range(field.shape[1]):
        field[index, t, place : place + line.shape[0], :] = line[:, t * LANES : (t + 1) * LANES]


def set_row(field, index, place, line):
    for t in range(field.shape[1]):
        field[index, t, place : place + 1, :] = line[:, t * LANES : (t + 1) * LANES]


def set_edges(field, slices, strip, strips, up, down, edges):
    for index, block, _ in slices:
        widen(field, index, up[block], 0)
        widen(field, index, down[block], 8 + ROWS)
    if not edges:
        return
    for edge, last, place in ((edges[0], 0, 7), (edges[1], strips - 1, 8 + ROWS)):

        @pl.when(strip == last)
        def _(edge=edge, place=place):
            line = edge[...].astype(jnp.float32)
            for index, _, s in slices:
                set_row(field, index, place, line[s : s + 1])


def clear_edges(moved_v, moved_s):
    @pl.when(pl.program_id(0) == 0)
    def _():
        tiles = moved_v.shape[1] - 2
        zero = jnp.zeros((moved_v.shape[0], ROWS, LANES), jnp.float32)
        for t in (0, tiles + 1):
            moved_v[:, t] = zero
            moved_s[:, t] = zero


def emit(state, outs, slot, group, part, count):
    for j in range(count):
        at = pl.ds(pl.multiple_of((part * count + j) * LANES, LANES), LANES)
        clear, total, colours = state[j]
        for c in range(3):
            outs[slot][group, c, :, at] = (total + colours[c]).astype(jnp.bfloat16)
        outs[slot][group, 3, :, at] = (1.0 - clear).astype(jnp.bfloat16)


def over_columns(outs, me, inner, body):
    groups, _, _, width = outs[0].shape
    per = width // LANES
    count = min(2, per)
    for slot in range(inner):
        column = lax.rem(lax.rem(me, inner) + slot, inner)

        def column_step(i, carry, slot=slot, column=column):
            group, part = i // (per // count), lax.rem(i, per // count)
            first = (group * inner + column) * per + part * count
            emit(body(first, count), outs, slot, group, part, count)
            return carry

        lax.fori_loop(0, groups * (per // count), column_step, 0)


def inner_kernel(absorb, strip_of, strips, shear, footprint, vol, up, down, *refs):
    edges, (out, field, moved_v, moved_s) = refs[:-4], refs[-4:]
    slices, _, ny = vol.shape
    me = lax.axis_index("depth")
    flip = shear[0] > shear[shear.shape[0] - 1]
    clear_edges(moved_v, moved_s)
    centre = [(s, s, s) for s in range(1, slices - 1)]
    set_edges(field, centre, strip_of(pl.program_id(0)), strips, up, down, edges)

    def widen_step(s, carry):
        widen(field, s, vol[s], 8)
        return carry

    lax.fori_loop(0, slices, widen_step, 0)

    def shade_step(i, carry):
        narrow = lambda t: vol[i + 1, :, t * LANES : (t + 1) * LANES]
        shift = shear[me * slices + i + 1]
        shade_slice(field, moved_v, moved_s, i + 1, shift, i, 0, narrow)
        return carry

    lax.fori_loop(0, slices - 2, shade_step, 0)

    def column_step(pair, carry):
        first = 2 * pair
        rate = rates(absorb, footprint, first, 2)
        state = fresh(2)
        for step in range(slices - 2):
            i = jnp.where(flip, slices - 3 - step, step)
            shift = shear[me * slices + i + 1]
            state = blend(state, moved_v, moved_s, i, shift, first, 2, rate)
        for j in range(2):
            at = pl.ds(pl.multiple_of((first + j) * LANES, LANES), LANES)
            clear, total, colours = state[j]
            for c in range(3):
                out[c, :, at] = total + colours[c]
            out[3, :, at] = clear
        return carry

    lax.fori_loop(0, ny // LANES // 2, column_step, 0)


def outer_kernel(absorb, inner, strip_of, strips, shear, footprint, *refs):
    front, back, front_up, front_down, back_up, back_down, prev, nxt, mid = refs[:9]
    edges, outs, (field, moved_v, moved_s) = refs[9 : -3 - inner], refs[-3 - inner : -3], refs[-3:]
    me = lax.axis_index("depth")
    flip = shear[0] > shear[shear.shape[0] - 1]
    slices = shear.shape[0] // lax.axis_size("depth")
    strip = strip_of(pl.program_id(0))
    clear_edges(moved_v, moved_s)
    set_edges(field, [(1, 0, 0)], strip, strips, front_up, front_down, edges)
    set_edges(field, [(4, 0, slices - 1)], strip, strips, back_up, back_down, edges)
    for index, line in enumerate((prev, front.at[0], front.at[1], back.at[0], back.at[1], nxt)):
        widen(field, index, line[...], 8)
    for i, ref in ((0, front.at[0]), (1, back.at[1])):
        narrow = lambda t, ref=ref: ref[:, t * LANES : (t + 1) * LANES]
        shift = shear[me * slices + i * (slices - 1)]
        shade_slice(field, moved_v, moved_s, 1 + 3 * i, shift, i, 0, narrow)

    def column(first, count):
        rate = rates(absorb, footprint, first, count)
        state = fresh(count)
        for step in range(2):
            i = jnp.where(flip, 1 - step, step)
            shift = shear[me * slices + i * (slices - 1)]
            state = blend(state, moved_v, moved_s, i, shift, first, count, rate)
            if step == 0:
                for j in range(count):
                    at = pl.ds(pl.multiple_of((first + j) * LANES, LANES), LANES)
                    clear, total, colours = state[j]
                    colours = [colours[c] + clear * mid[c, :, at] for c in range(3)]
                    state[j] = (clear * mid[3, :, at], total, colours)
        return state

    over_columns(outs, me, inner, column)


def full_kernel(absorb, inner, strip_of, strips, shear, footprint, vol, up, down, prev, nxt, *refs):
    edges, outs, (field, moved_v, moved_s) = refs[: -3 - inner], refs[-3 - inner : -3], refs[-3:]
    slices = vol.shape[0]
    me = lax.axis_index("depth")
    flip = shear[0] > shear[shear.shape[0] - 1]
    clear_edges(moved_v, moved_s)
    centre = [(s + 1, s, s) for s in range(slices)]
    set_edges(field, centre, strip_of(pl.program_id(0)), strips, up, down, edges)

    def widen_step(s, carry):
        widen(field, s + 1, vol[s], 8)
        return carry

    lax.fori_loop(0, slices, widen_step, 0)
    widen(field, 0, prev[...], 8)
    widen(field, slices + 1, nxt[...], 8)

    def shade_step(i, carry):
        narrow = lambda t: vol[i, :, t * LANES : (t + 1) * LANES]
        shade_slice(field, moved_v, moved_s, i + 1, shear[me * slices + i], i, 0, narrow)
        return carry

    lax.fori_loop(0, slices, shade_step, 0)

    def column(first, count):
        rate = rates(absorb, footprint, first, count)
        state = fresh(count)
        for step in range(slices):
            i = jnp.where(flip, slices - 1 - step, step)
            shift = shear[me * slices + i]
            state = blend(state, moved_v, moved_s, i, shift, first, count, rate)
        return state

    over_columns(outs, me, inner, column)


def encode(x):
    x = jnp.maximum(x, 1e-30)
    code = (x * lax.rsqrt(x) * 65535.0 + 0.5).astype(jnp.int32) - 32768
    return code.astype(LINK)


def decode(code):
    root = (code.astype(jnp.int32) + 32768).astype(jnp.float32) * (1.0 / 65535.0)
    return root * root


def over(pieces):
    image = pieces[0]
    for piece in pieces[1:]:
        clear = 1.0 - image[3]
        image = [image[c] + clear * piece[c] for c in range(4)]
    return image


def ordered(count, mine, flip, body):
    cases = {}
    for position in range(count):
        for turned in (False, True):
            order = tuple((position - p) % count for p in range(count))
            cases.setdefault(order[::-1] if turned else order, []).append((position, turned))
    for order, where in cases.items():
        chosen = functools.reduce(
            jnp.logical_or, [(mine == position) & (flip == turned) for position, turned in where]
        )
        pl.when(chosen)(functools.partial(body, order))


def group_kernel(inner, shear, *refs):
    sources, outs = refs[:inner], refs[inner:]
    me = lax.axis_index("depth")
    flip = shear[0] > shear[shear.shape[0] - 1]
    groups = len(outs)

    def body(order):
        for k in range(groups):
            target = lax.rem(lax.div(me, inner) + k, groups)
            pieces = [
                [sources[shift][target, c].astype(jnp.float32) for c in range(4)]
                for shift in order
            ]
            for c, value in enumerate(over(pieces)):
                outs[k][c] = encode(value)

    ordered(inner, lax.rem(me, inner), flip, body)


def frame_kernel(inner, aliased, shear, *refs):
    sources, out = refs[:-1], refs[-1]
    if aliased:
        sources = sources[:-1]
    me = lax.axis_index("depth")
    flip = shear[0] > shear[shear.shape[0] - 1]

    def body(order):
        pieces = [[decode(sources[shift][c]) for c in range(4)] for shift in order]
        for c, value in enumerate(over(pieces)):
            out[c] = value

    ordered(len(sources), lax.div(me, inner), flip, body)


def shards(volume, shear, footprint):
    slices, rows, ny = volume.shape
    bricks = lax.axis_size("depth")
    crosswise = lax.axis_size("tile")
    absorb = 2.0 / (slices * bricks)
    inner = 1
    while 4 * inner * inner <= bricks:
        inner *= 2
    groups = bricks // inner
    width = ny // bricks
    tiles = ny // LANES
    strips = rows // ROWS

    def line(length):
        return [(i, i + 1) for i in range(length - 1)], [(i + 1, i) for i in range(length - 1)]

    depth_up, depth_down = line(bricks)
    row_up, row_down = line(crosswise)

    parts = [(1, 1, strips - 2)] if strips > 2 else []
    parts += [(0, max(strips - 1, 1), min(strips, 2))]

    def rows_of(part, s):
        first, step, count = part
        cut = volume[s].reshape(strips, ROWS, ny)[first : first + step * (count - 1) + 1 : step]
        return cut.reshape(count * ROWS, ny)

    halos = [
        (
            lax.ppermute(rows_of(part, slices - 1), "depth", depth_up),
            lax.ppermute(rows_of(part, 0), "depth", depth_down),
        )
        for part in parts
    ]
    above = lax.ppermute(volume[:, rows - 1, :], "tile", row_up)
    below = lax.ppermute(volume[:, 0, :], "tile", row_down)

    vmem = pl.BlockSpec(memory_space=pltpu.VMEM)
    smem = pl.BlockSpec(memory_space=pltpu.SMEM)
    anywhere = pl.BlockSpec(memory_space=pl.ANY)
    moved = lambda n: pltpu.VMEM((n, tiles + 2, ROWS, LANES), jnp.float32)
    field = lambda n: pltpu.VMEM((n, tiles, ROWS + 16, LANES), jnp.float32)
    flat = pl.BlockSpec((ROWS, ny), lambda i: (i, 0))
    received = []
    for number, part in enumerate(parts):
        first, step, count = part
        chunk = count * ROWS
        strip_of = lambda i, first=first, step=step: first + step * i
        prev, nxt = halos[number]
        edges = [above, below] if number == len(parts) - 1 else []

        def slab(size, s, move=0, strip_of=strip_of):
            if move == 0:
                return pl.BlockSpec((size, ROWS, ny), lambda i: (s, strip_of(i), 0))
            offset = -1 if move < 0 else ROWS // 8

            def index(i):
                return s, jnp.clip(strip_of(i) * (ROWS // 8) + offset, 0, rows // 8 - 1), 0

            return pl.BlockSpec((size, 8, ny), index)

        def cost(per, chunk=chunk):
            return pl.CostEstimate(
                flops=per * chunk * ny, bytes_accessed=chunk * ny * 32, transcendentals=0
            )

        side_shape = [jax.ShapeDtypeStruct((groups, 4, chunk, width), jnp.bfloat16)] * inner
        side_spec = [pl.BlockSpec((groups, 4, ROWS, width), lambda i: (0, 0, i, 0))] * inner
        whole = [slab(slices, 0), slab(slices, 0, -1), slab(slices, 0, 1)]
        if number < len(parts) - 1:
            middle = pl.BlockSpec((4, ROWS, ny), lambda i: (0, i, 0))
            mid = pl.pallas_call(
                functools.partial(inner_kernel, absorb, strip_of, strips),
                out_shape=jax.ShapeDtypeStruct((4, chunk, ny), jnp.float32),
                grid=(count,),
                in_specs=[smem, smem] + whole + [vmem] * len(edges),
                out_specs=middle,
                scratch_shapes=[field(slices), moved(slices - 2), moved(slices - 2)],
                cost_estimate=cost(800),
                compiler_params=params(INNER_MIB),
                name="inner",
            )(shear, footprint, *[volume] * 3, *edges)
            sides = pl.pallas_call(
                functools.partial(outer_kernel, absorb, inner, strip_of, strips),
                out_shape=side_shape,
                grid=(count,),
                in_specs=[smem, smem, slab(2, 0), slab(2, slices // 2 - 1)]
                + [slab(1, 0, -1), slab(1, 0, 1), slab(1, slices - 1, -1), slab(1, slices - 1, 1)]
                + [flat, flat, middle]
                + [vmem] * len(edges),
                out_specs=side_spec,
                scratch_shapes=[field(6), moved(2), moved(2)],
                cost_estimate=cost(400),
                compiler_params=params(OUTER_MIB),
                name="outer",
            )(shear, footprint, *[volume] * 6, prev, nxt, mid, *edges)
        else:
            sides = pl.pallas_call(
                functools.partial(full_kernel, absorb, inner, strip_of, strips),
                out_shape=side_shape,
                grid=(count,),
                in_specs=[smem, smem] + whole + [flat, flat] + [vmem] * len(edges),
                out_specs=side_spec,
                scratch_shapes=[field(slices + 2), moved(slices), moved(slices)],
                cost_estimate=cost(1100),
                compiler_params=params(OUTER_MIB),
                name="full",
            )(shear, footprint, *[volume] * 3, prev, nxt, *edges)
        sides = list(sides)
        for k in range(1, inner):
            pairs = [
                (g * inner + x, g * inner + (x + k) % inner)
                for g in range(groups)
                for x in range(inner)
            ]
            sides[k] = lax.ppermute(sides[k], "depth", pairs)
        received.append(sides)

    frame = None
    for (first, step, count), sides in zip(parts, received):
        chunk = count * ROWS
        pieces = pl.pallas_call(
            functools.partial(group_kernel, inner),
            out_shape=[jax.ShapeDtypeStruct((4, chunk, width), LINK)] * groups,
            grid=(count,),
            in_specs=[smem]
            + [pl.BlockSpec((groups, 4, ROWS, width), lambda i: (0, 0, i, 0))] * inner,
            out_specs=[pl.BlockSpec((4, ROWS, width), lambda i: (0, i, 0))] * groups,
            cost_estimate=pl.CostEstimate(
                flops=20 * chunk * ny, bytes_accessed=2 << 20, transcendentals=0
            ),
            compiler_params=params(16),
            name="group",
        )(shear, *sides)
        pieces = list(pieces)
        for k in range(1, groups):
            pairs = [
                (g * inner + x, (g + k) % groups * inner + x)
                for g in range(groups)
                for x in range(inner)
            ]
            pieces[k] = lax.ppermute(pieces[k], "depth", pairs)
        frame = pl.pallas_call(
            functools.partial(frame_kernel, inner, frame is not None),
            out_shape=jax.ShapeDtypeStruct((4, rows, width), jnp.float32),
            grid=(count,),
            in_specs=[smem]
            + [pl.BlockSpec((4, ROWS, width), lambda i: (0, i, 0))] * groups
            + [anywhere] * (frame is not None),
            out_specs=pl.BlockSpec(
                (4, ROWS, width), lambda i, first=first, step=step: (0, first + step * i, 0)
            ),
            input_output_aliases={} if frame is None else {1 + groups: 0},
            cost_estimate=pl.CostEstimate(
                flops=20 * chunk * width, bytes_accessed=2 << 20, transcendentals=0
            ),
            compiler_params=params(16),
            name="frame",
        )(shear, *pieces, *([] if frame is None else [frame]))
    return frame


def solution(mesh):
    placed = (P("depth", "tile", None), P(), P("depth", None))
    return jax.shard_map(
        shards, mesh=mesh, in_specs=placed, out_specs=P(None, "tile", "depth"), check_vma=False
    )
```

```python
import functools

import jax
import jax.numpy as jnp
from jax import lax
from jax.experimental import pallas as pl
from jax.experimental.pallas import tpu as pltpu
from jax.sharding import PartitionSpec as P


LANES = 128
ROWS = 16
LOG2E = 1.4426950408889634
LINK = jnp.int16
PARTS = 2


def params(mib):
    return pltpu.CompilerParams(vmem_limit_bytes=mib << 20)


def shade_slice(field, moved_v, moved_s, where, shift, base, r, narrow):
    tiles = field.shape[1]
    lane = lax.broadcasted_iota(jnp.int32, (ROWS, LANES), 1)
    leftmost, rightmost = lane == 0, lane == LANES - 1
    turn = jnp.where(shift < 0, shift + LANES, shift)
    here, up, down = pl.ds(r + 8, ROWS), pl.ds(r + 7, ROWS), pl.ds(r + 9, ROWS)
    zero = jnp.zeros((ROWS, LANES), jnp.float32)
    v = field[where, 0, here, :]
    ahead = pltpu.roll(v, LANES - 1, 1)
    behind_last = zero
    for t in range(tiles):
        v_next = field[where, t + 1, here, :] if t + 1 < tiles else zero
        ahead_next = pltpu.roll(v_next, LANES - 1, 1) if t + 1 < tiles else zero
        behind = pltpu.roll(v, 1, 1)
        dy = jnp.where(rightmost, ahead_next, ahead) - jnp.where(leftmost, behind_last, behind)
        dz = field[where + 1, t, here, :] - field[where - 1, t, here, :]
        dx = field[where, t, down, :] - field[where, t, up, :]
        squares = (dx * dx + dy * dy) + (dz * dz + 4.0)
        along = (0.35 * 0.48) * dx + (0.35 * 0.6) * dy + (0.35 * 0.64) * dz
        moved_s[base, t + 1] = 0.15 + jnp.abs(along) * lax.rsqrt(squares)
        v, ahead, behind_last = v_next, ahead_next, behind

    def turn_step(once, carry):
        for t in range(tiles):
            moved_v[base, t + 1] = pltpu.roll(narrow(t), turn, 1).astype(jnp.float32)
            moved_s[base, t + 1] = pltpu.roll(moved_s[base, t + 1], turn, 1)
        return carry

    lax.fori_loop(0, 1 + jnp.minimum(turn, 0), turn_step, 0)


def blend(state, moved_v, moved_s, index, shift, first, count, rate):
    lane = lax.broadcasted_iota(jnp.int32, (ROWS, LANES), 1)
    turn = jnp.where(shift < 0, shift + LANES, shift)
    start = first + jnp.where(shift < 0, 1, 0)
    keep = lane < turn
    values = [moved_v[index, start + j] for j in range(count + 1)]
    shades = [moved_s[index, start + j] for j in range(count + 1)]
    result = []
    for j in range(count):
        clear, total, colours = state[j]
        v = jnp.where(keep, values[j], values[j + 1])
        half = jnp.where(keep, shades[j], shades[j + 1])
        left = clear * jnp.exp2(v * v * rate[j])
        weight = (clear - left) * half
        arguments = (0.6 * v + 0.1, -0.4 * v, 0.25 * v - 0.15)
        colours = [colours[c] + weight * jnp.tanh(arguments[c]) for c in range(3)]
        result.append((left, total + weight, colours))
    return result


def rates(absorb, footprint, first, count):
    lane = lax.broadcasted_iota(jnp.int32, (ROWS, LANES), 1)
    found = []
    for j in range(count):
        column = lane + (first + j) * LANES
        inside = (column >= footprint[0, 0]) & (column < footprint[0, 1])
        found.append(jnp.where(inside, -absorb * LOG2E, 0.0))
    return found


def fresh(count):
    zero = jnp.zeros((ROWS, LANES), jnp.float32)
    return [(zero + 1.0, zero, [zero] * 3) for _ in range(count)]


def widen(field, index, line, r):
    line = line.astype(jnp.float32)
    for t in range(field.shape[1]):
        field[index, t, pl.ds(r + 8, ROWS), :] = line[:, t * LANES : (t + 1) * LANES]


def set_row(field, index, place, line):
    for t in range(field.shape[1]):
        field[index, t, place : place + 1, :] = line[:, t * LANES : (t + 1) * LANES]


def clear_edges(moved_v, moved_s):
    tiles = moved_v.shape[1] - 2
    zero = jnp.zeros((moved_v.shape[0], ROWS, LANES), jnp.float32)
    for t in (0, tiles + 1):
        moved_v[:, t] = zero
        moved_s[:, t] = zero


def inner_kernel(
    absorb, shear, footprint, vol, above, below, out, field, moved_v, moved_s, held, arrived
):
    slices, rows, ny = vol.shape
    me = lax.axis_index("depth")
    flip = shear[0] > shear[shear.shape[0] - 1]
    tiles = ny // LANES
    strips = rows // ROWS
    strip = pl.program_id(0)
    r = pl.multiple_of(strip * ROWS, ROWS)

    def strip_copy(k):
        at = pl.ds(pl.multiple_of(k * ROWS, ROWS), ROWS)
        return pltpu.make_async_copy(vol.at[:, at, :], held.at[:, at, :], arrived.at[k])

    def widen_strip(k):
        at = pl.multiple_of(k * ROWS, ROWS)

        def widen_step(s, carry):
            widen(field, s, held[s, pl.ds(at, ROWS), :], at)
            return carry

        lax.fori_loop(0, slices, widen_step, 0)

    @pl.when(strip == 0)
    def _():
        for k in range(strips):
            strip_copy(k).start()
        clear_edges(moved_v, moved_s)
        top = above[...].astype(jnp.float32)
        bottom = below[...].astype(jnp.float32)
        for s in range(1, slices - 1):
            set_row(field, s, 7, top[s : s + 1])
            set_row(field, s, 8 + rows, bottom[s : s + 1])
        strip_copy(0).wait()
        widen_strip(0)

    @pl.when(strip + 1 < strips)
    def _():
        strip_copy(strip + 1).wait()
        widen_strip(strip + 1)

    def shade_step(i, carry):
        narrow = lambda t: held[i + 1, pl.ds(r, ROWS), t * LANES : (t + 1) * LANES]
        shift = shear[me * slices + i + 1]
        shade_slice(field, moved_v, moved_s, i + 1, shift, i, r, narrow)
        return carry

    lax.fori_loop(0, slices - 2, shade_step, 0)

    def column_step(pair, carry):
        first = 2 * pair
        rate = rates(absorb, footprint, first, 2)
        state = fresh(2)
        for step in range(slices - 2):
            i = jnp.where(flip, slices - 3 - step, step)
            shift = shear[me * slices + i + 1]
            state = blend(state, moved_v, moved_s, i, shift, first, 2, rate)
        for j in range(2):
            at = pl.ds(pl.multiple_of((first + j) * LANES, LANES), LANES)
            clear, total, colours = state[j]
            for c in range(3):
                out[c, :, at] = total + colours[c]
            out[3, :, at] = clear
        return carry

    lax.fori_loop(0, tiles // 2, column_step, 0)


def outer_kernel(absorb, inner, row0, rows, shear, footprint, *refs):
    front, back, front_up, front_down, back_up, back_down, above, below, prev, nxt, mid = refs[:11]
    outs, (field, moved_v, moved_s) = refs[11 : 11 + inner], refs[11 + inner :]
    slices = above.shape[0]
    groups, _, _, width = outs[0].shape
    me = lax.axis_index("depth")
    flip = shear[0] > shear[shear.shape[0] - 1]
    r = row0 + pl.program_id(0) * ROWS

    @pl.when(pl.program_id(0) == 0)
    def _():
        clear_edges(moved_v, moved_s)

    for index, up, down, s in ((1, front_up, front_down, 0), (4, back_up, back_down, slices - 1)):
        at_top, at_bottom = r == 0, r + ROWS == rows
        over_line = up[0].astype(jnp.float32)[ROWS - 1 : ROWS]
        under_line = down[0].astype(jnp.float32)[0:1]
        over_edge = above[...].astype(jnp.float32)[s : s + 1]
        under_edge = below[...].astype(jnp.float32)[s : s + 1]
        set_row(field, index, 7, jnp.where(at_top, over_edge, over_line))
        set_row(field, index, 8 + ROWS, jnp.where(at_bottom, under_edge, under_line))
    for index, line in enumerate((prev, front.at[0], front.at[1], back.at[0], back.at[1], nxt)):
        widen(field, index, line[...], 0)
    for i, ref in ((0, front.at[0]), (1, back.at[1])):
        narrow = lambda t, ref=ref: ref[:, t * LANES : (t + 1) * LANES]
        shift = shear[me * slices + i * (slices - 1)]
        shade_slice(field, moved_v, moved_s, 1 + 3 * i, shift, i, 0, narrow)
    per = width // LANES
    count = min(2, per)
    for slot in range(inner):
        column = lax.rem(lax.rem(me, inner) + slot, inner)

        def column_step(i, carry, slot=slot, column=column):
            group, part = i // (per // count), lax.rem(i, per // count)
            first = (group * inner + column) * per + part * count
            rate = rates(absorb, footprint, first, count)
            state = fresh(count)
            for step in range(2):
                i = jnp.where(flip, 1 - step, step)
                shift = shear[me * slices + i * (slices - 1)]
                state = blend(state, moved_v, moved_s, i, shift, first, count, rate)
                if step == 0:
                    for j in range(count):
                        at = pl.ds(pl.multiple_of((first + j) * LANES, LANES), LANES)
                        clear, total, colours = state[j]
                        colours = [colours[c] + clear * mid[c, :, at] for c in range(3)]
                        state[j] = (clear * mid[3, :, at], total, colours)
            for j in range(count):
                at = pl.ds(pl.multiple_of((part * count + j) * LANES, LANES), LANES)
                clear, total, colours = state[j]
                for c in range(3):
                    outs[slot][group, c, :, at] = (total + colours[c]).astype(jnp.bfloat16)
                outs[slot][group, 3, :, at] = (1.0 - clear).astype(jnp.bfloat16)
            return carry

        lax.fori_loop(0, groups * (per // count), column_step, 0)


def encode(x):
    x = jnp.maximum(x, 1e-30)
    code = (x * lax.rsqrt(x) * 65535.0 + 0.5).astype(jnp.int32) - 32768
    return code.astype(LINK)


def decode(code):
    root = (code.astype(jnp.int32) + 32768).astype(jnp.float32) * (1.0 / 65535.0)
    return root * root


def over(pieces):
    image = pieces[0]
    for piece in pieces[1:]:
        clear = 1.0 - image[3]
        image = [image[c] + clear * piece[c] for c in range(4)]
    return image


def ordered(count, mine, flip, body):
    cases = {}
    for position in range(count):
        for turned in (False, True):
            order = tuple((position - p) % count for p in range(count))
            cases.setdefault(order[::-1] if turned else order, []).append((position, turned))
    for order, where in cases.items():
        chosen = functools.reduce(
            jnp.logical_or, [(mine == position) & (flip == turned) for position, turned in where]
        )
        pl.when(chosen)(functools.partial(body, order))


def group_kernel(inner, shear, *refs):
    sources, outs = refs[:inner], refs[inner:]
    me = lax.axis_index("depth")
    flip = shear[0] > shear[shear.shape[0] - 1]
    groups = len(outs)

    def body(order):
        for k in range(groups):
            target = lax.rem(lax.div(me, inner) + k, groups)
            pieces = [
                [sources[shift][target, c].astype(jnp.float32) for c in range(4)]
                for shift in order
            ]
            for c, value in enumerate(over(pieces)):
                outs[k][c] = encode(value)

    ordered(inner, lax.rem(me, inner), flip, body)


def frame_kernel(inner, aliased, shear, *refs):
    sources, out = refs[:-1], refs[-1]
    if aliased:
        sources = sources[:-1]
    me = lax.axis_index("depth")
    flip = shear[0] > shear[shear.shape[0] - 1]

    def body(order):
        pieces = [[decode(sources[shift][c]) for c in range(4)] for shift in order]
        for c, value in enumerate(over(pieces)):
            out[c] = value

    ordered(len(sources), lax.div(me, inner), flip, body)


def shards(volume, shear, footprint):
    slices, rows, ny = volume.shape
    bricks = lax.axis_size("depth")
    crosswise = lax.axis_size("tile")
    absorb = 2.0 / (slices * bricks)
    inner = 1
    while 4 * inner * inner <= bricks:
        inner *= 2
    groups = bricks // inner
    width = ny // bricks
    tiles = ny // LANES
    strips = rows // ROWS

    def line(length):
        return [(i, i + 1) for i in range(length - 1)], [(i + 1, i) for i in range(length - 1)]

    depth_up, depth_down = line(bricks)
    row_up, row_down = line(crosswise)
    above = lax.ppermute(volume[:, rows - 1, :], "tile", row_up)
    below = lax.ppermute(volume[:, 0, :], "tile", row_down)
    prev = lax.ppermute(volume[slices - 1], "depth", depth_up)
    nxt = lax.ppermute(volume[0], "depth", depth_down)

    vmem = pl.BlockSpec(memory_space=pltpu.VMEM)
    smem = pl.BlockSpec(memory_space=pltpu.SMEM)
    anywhere = pl.BlockSpec(memory_space=pl.ANY)
    moved = lambda n: pltpu.VMEM((n, tiles + 2, ROWS, LANES), jnp.float32)
    mid = pl.pallas_call(
        functools.partial(inner_kernel, absorb),
        out_shape=jax.ShapeDtypeStruct((4, rows, ny), jnp.float32),
        grid=(strips,),
        in_specs=[smem, smem, pl.BlockSpec(memory_space=pltpu.HBM), vmem, vmem],
        out_specs=pl.BlockSpec((4, ROWS, ny), lambda i: (0, i, 0)),
        scratch_shapes=[
            pltpu.VMEM((slices, tiles, rows + 20, LANES), jnp.float32),
            moved(slices - 2),
            moved(slices - 2),
            pltpu.VMEM((slices, rows, ny), jnp.bfloat16),
            pltpu.SemaphoreType.DMA((strips,)),
        ],
        cost_estimate=pl.CostEstimate(
            flops=100 * slices * rows * ny, bytes_accessed=8 << 20, transcendentals=0
        ),
        compiler_params=params(48),
        name="inner",
    )(shear, footprint, volume, above, below)

    chunk = rows // PARTS
    frame = None
    for part in range(PARTS):
        row0 = part * chunk
        strip0 = row0 // ROWS

        def slab(size, s, move=0, strip0=strip0):
            def index(i):
                return s, jnp.clip(strip0 + i + move, 0, strips - 1), 0

            return pl.BlockSpec((size, ROWS, ny), index)

        flat = pl.BlockSpec((ROWS, ny), lambda i, strip0=strip0: (strip0 + i, 0))
        sides = pl.pallas_call(
            functools.partial(outer_kernel, absorb, inner, row0, rows),
            out_shape=[jax.ShapeDtypeStruct((groups, 4, chunk, width), jnp.bfloat16)] * inner,
            grid=(chunk // ROWS,),
            in_specs=[
                smem,
                smem,
                slab(2, 0),
                slab(2, slices // 2 - 1),
                slab(1, 0, -1),
                slab(1, 0, 1),
                slab(1, slices - 1, -1),
                slab(1, slices - 1, 1),
                vmem,
                vmem,
                flat,
                flat,
                pl.BlockSpec((4, ROWS, ny), lambda i, strip0=strip0: (0, strip0 + i, 0)),
            ],
            out_specs=[pl.BlockSpec((groups, 4, ROWS, width), lambda i: (0, 0, i, 0))] * inner,
            scratch_shapes=[pltpu.VMEM((6, tiles, 36, LANES), jnp.float32), moved(2), moved(2)],
            cost_estimate=pl.CostEstimate(
                flops=200 * chunk * ny, bytes_accessed=4 << 20, transcendentals=0
            ),
            compiler_params=params(24),
            name="outer",
        )(shear, footprint, *[volume] * 6, above, below, prev, nxt, mid)
        sides = list(sides)
        for k in range(1, inner):
            pairs = [
                (g * inner + x, g * inner + (x + k) % inner)
                for g in range(groups)
                for x in range(inner)
            ]
            sides[k] = lax.ppermute(sides[k], "depth", pairs)
        pieces = pl.pallas_call(
            functools.partial(group_kernel, inner),
            out_shape=[jax.ShapeDtypeStruct((4, chunk, width), LINK)] * groups,
            grid=(chunk // ROWS,),
            in_specs=[smem]
            + [pl.BlockSpec((groups, 4, ROWS, width), lambda i: (0, 0, i, 0))] * inner,
            out_specs=[pl.BlockSpec((4, ROWS, width), lambda i: (0, i, 0))] * groups,
            cost_estimate=pl.CostEstimate(
                flops=20 * chunk * ny, bytes_accessed=2 << 20, transcendentals=0
            ),
            compiler_params=params(16),
            name="group",
        )(shear, *sides)
        pieces = list(pieces)
        for k in range(1, groups):
            pairs = [
                (g * inner + x, (g + k) % groups * inner + x)
                for g in range(groups)
                for x in range(inner)
            ]
            pieces[k] = lax.ppermute(pieces[k], "depth", pairs)
        frame = pl.pallas_call(
            functools.partial(frame_kernel, inner, frame is not None),
            out_shape=jax.ShapeDtypeStruct((4, rows, width), jnp.float32),
            grid=(chunk // ROWS,),
            in_specs=[smem]
            + [pl.BlockSpec((4, ROWS, width), lambda i: (0, i, 0))] * groups
            + [anywhere] * (frame is not None),
            out_specs=pl.BlockSpec((4, ROWS, width), lambda i, strip0=strip0: (0, strip0 + i, 0)),
            input_output_aliases={} if frame is None else {1 + groups: 0},
            cost_estimate=pl.CostEstimate(
                flops=20 * chunk * width, bytes_accessed=2 << 20, transcendentals=0
            ),
            compiler_params=params(16),
            name="frame",
        )(shear, *pieces, *([] if frame is None else [frame]))
    return frame


def solution(mesh):
    placed = (P("depth", "tile", None), P(), P("depth", None))
    return jax.shard_map(
        shards, mesh=mesh, in_specs=placed, out_specs=P(None, "tile", "depth"), check_vma=False
    )
```

```python
import functools

import jax
import jax.numpy as jnp
from jax import lax
from jax.experimental import pallas as pl
from jax.experimental.pallas import tpu as pltpu
from jax.sharding import PartitionSpec as P


LANES = 128
ROWS = 16
LOG2E = 1.4426950408889634
LINK = jnp.int16
INNER_MIB = 48
OUTER_MIB = 24


def params(mib):
    return pltpu.CompilerParams(vmem_limit_bytes=mib << 20)


def shade_slice(field, moved_v, moved_s, where, shift, base, r, narrow):
    tiles = field.shape[1]
    lane = lax.broadcasted_iota(jnp.int32, (ROWS, LANES), 1)
    leftmost, rightmost = lane == 0, lane == LANES - 1
    turn = jnp.where(shift < 0, shift + LANES, shift)
    here, up, down = pl.ds(r + 8, ROWS), pl.ds(r + 7, ROWS), pl.ds(r + 9, ROWS)
    zero = jnp.zeros((ROWS, LANES), jnp.float32)
    v = field[where, 0, here, :]
    ahead = pltpu.roll(v, LANES - 1, 1)
    behind_last = zero
    for t in range(tiles):
        v_next = field[where, t + 1, here, :] if t + 1 < tiles else zero
        ahead_next = pltpu.roll(v_next, LANES - 1, 1) if t + 1 < tiles else zero
        behind = pltpu.roll(v, 1, 1)
        dy = jnp.where(rightmost, ahead_next, ahead) - jnp.where(leftmost, behind_last, behind)
        dz = field[where + 1, t, here, :] - field[where - 1, t, here, :]
        dx = field[where, t, down, :] - field[where, t, up, :]
        squares = (dx * dx + dy * dy) + (dz * dz + 4.0)
        along = (0.35 * 0.48) * dx + (0.35 * 0.6) * dy + (0.35 * 0.64) * dz
        moved_s[base, t + 1] = 0.15 + jnp.abs(along) * lax.rsqrt(squares)
        v, ahead, behind_last = v_next, ahead_next, behind

    def turn_step(once, carry):
        for t in range(tiles):
            moved_v[base, t + 1] = pltpu.roll(narrow(t), turn, 1).astype(jnp.float32)
            moved_s[base, t + 1] = pltpu.roll(moved_s[base, t + 1], turn, 1)
        return carry

    lax.fori_loop(0, 1 + jnp.minimum(turn, 0), turn_step, 0)


def blend(state, moved_v, moved_s, index, shift, first, count, rate):
    lane = lax.broadcasted_iota(jnp.int32, (ROWS, LANES), 1)
    turn = jnp.where(shift < 0, shift + LANES, shift)
    start = first + jnp.where(shift < 0, 1, 0)
    keep = lane < turn
    values = [moved_v[index, start + j] for j in range(count + 1)]
    shades = [moved_s[index, start + j] for j in range(count + 1)]
    result = []
    for j in range(count):
        clear, total, colours = state[j]
        v = jnp.where(keep, values[j], values[j + 1])
        half = jnp.where(keep, shades[j], shades[j + 1])
        left = clear * jnp.exp2(v * v * rate[j])
        weight = (clear - left) * half
        arguments = (0.6 * v + 0.1, -0.4 * v, 0.25 * v - 0.15)
        colours = [colours[c] + weight * jnp.tanh(arguments[c]) for c in range(3)]
        result.append((left, total + weight, colours))
    return result


def rates(absorb, footprint, first, count):
    lane = lax.broadcasted_iota(jnp.int32, (ROWS, LANES), 1)
    found = []
    for j in range(count):
        column = lane + (first + j) * LANES
        inside = (column >= footprint[0, 0]) & (column < footprint[0, 1])
        found.append(jnp.where(inside, -absorb * LOG2E, 0.0))
    return found


def fresh(count):
    zero = jnp.zeros((ROWS, LANES), jnp.float32)
    return [(zero + 1.0, zero, [zero] * 3) for _ in range(count)]


def widen(field, index, line, place):
    line = line.astype(jnp.float32)
    for t in range(field.shape[1]):
        field[index, t, place : place + line.shape[0], :] = line[:, t * LANES : (t + 1) * LANES]


def set_row(field, index, place, line):
    for t in range(field.shape[1]):
        field[index, t, place : place + 1, :] = line[:, t * LANES : (t + 1) * LANES]


def set_edges(field, slices, strip, strips, up, down, edges):
    for index, block, _ in slices:
        widen(field, index, up[block], 0)
        widen(field, index, down[block], 8 + ROWS)
    if not edges:
        return
    for edge, last, place in ((edges[0], 0, 7), (edges[1], strips - 1, 8 + ROWS)):

        @pl.when(strip == last)
        def _(edge=edge, place=place):
            line = edge[...].astype(jnp.float32)
            for index, _, s in slices:
                set_row(field, index, place, line[s : s + 1])


def clear_edges(moved_v, moved_s):
    @pl.when(pl.program_id(0) == 0)
    def _():
        tiles = moved_v.shape[1] - 2
        zero = jnp.zeros((moved_v.shape[0], ROWS, LANES), jnp.float32)
        for t in (0, tiles + 1):
            moved_v[:, t] = zero
            moved_s[:, t] = zero


def emit(state, outs, slot, group, part, count):
    for j in range(count):
        at = pl.ds(pl.multiple_of((part * count + j) * LANES, LANES), LANES)
        clear, total, colours = state[j]
        for c in range(3):
            outs[slot][group, c, :, at] = (total + colours[c]).astype(jnp.bfloat16)
        outs[slot][group, 3, :, at] = (1.0 - clear).astype(jnp.bfloat16)


def over_columns(outs, me, inner, body):
    groups, _, _, width = outs[0].shape
    per = width // LANES
    count = min(2, per)
    for slot in range(inner):
        column = lax.rem(lax.rem(me, inner) + slot, inner)

        def column_step(i, carry, slot=slot, column=column):
            group, part = i // (per // count), lax.rem(i, per // count)
            first = (group * inner + column) * per + part * count
            emit(body(first, count), outs, slot, group, part, count)
            return carry

        lax.fori_loop(0, groups * (per // count), column_step, 0)


def inner_kernel(absorb, strip_of, strips, shear, footprint, vol, up, down, *refs):
    edges, (out, field, moved_v, moved_s) = refs[:-4], refs[-4:]
    slices, _, ny = vol.shape
    me = lax.axis_index("depth")
    flip = shear[0] > shear[shear.shape[0] - 1]
    clear_edges(moved_v, moved_s)
    centre = [(s, s, s) for s in range(1, slices - 1)]
    set_edges(field, centre, strip_of(pl.program_id(0)), strips, up, down, edges)

    def widen_step(s, carry):
        widen(field, s, vol[s], 8)
        return carry

    lax.fori_loop(0, slices, widen_step, 0)

    def shade_step(i, carry):
        narrow = lambda t: vol[i + 1, :, t * LANES : (t + 1) * LANES]
        shift = shear[me * slices + i + 1]
        shade_slice(field, moved_v, moved_s, i + 1, shift, i, 0, narrow)
        return carry

    lax.fori_loop(0, slices - 2, shade_step, 0)

    def column_step(pair, carry):
        first = 2 * pair
        rate = rates(absorb, footprint, first, 2)
        state = fresh(2)
        for step in range(slices - 2):
            i = jnp.where(flip, slices - 3 - step, step)
            shift = shear[me * slices + i + 1]
            state = blend(state, moved_v, moved_s, i, shift, first, 2, rate)
        for j in range(2):
            at = pl.ds(pl.multiple_of((first + j) * LANES, LANES), LANES)
            clear, total, colours = state[j]
            for c in range(3):
                out[c, :, at] = total + colours[c]
            out[3, :, at] = clear
        return carry

    lax.fori_loop(0, ny // LANES // 2, column_step, 0)


def outer_kernel(absorb, inner, strip_of, strips, shear, footprint, *refs):
    front, back, front_up, front_down, back_up, back_down, prev, nxt, mid = refs[:9]
    edges, outs, (field, moved_v, moved_s) = refs[9 : -3 - inner], refs[-3 - inner : -3], refs[-3:]
    me = lax.axis_index("depth")
    flip = shear[0] > shear[shear.shape[0] - 1]
    slices = shear.shape[0] // lax.axis_size("depth")
    strip = strip_of(pl.program_id(0))
    clear_edges(moved_v, moved_s)
    set_edges(field, [(1, 0, 0)], strip, strips, front_up, front_down, edges)
    set_edges(field, [(4, 0, slices - 1)], strip, strips, back_up, back_down, edges)
    for index, line in enumerate((prev, front.at[0], front.at[1], back.at[0], back.at[1], nxt)):
        widen(field, index, line[...], 8)
    for i, ref in ((0, front.at[0]), (1, back.at[1])):
        narrow = lambda t, ref=ref: ref[:, t * LANES : (t + 1) * LANES]
        shift = shear[me * slices + i * (slices - 1)]
        shade_slice(field, moved_v, moved_s, 1 + 3 * i, shift, i, 0, narrow)

    def column(first, count):
        rate = rates(absorb, footprint, first, count)
        state = fresh(count)
        for step in range(2):
            i = jnp.where(flip, 1 - step, step)
            shift = shear[me * slices + i * (slices - 1)]
            state = blend(state, moved_v, moved_s, i, shift, first, count, rate)
            if step == 0:
                for j in range(count):
                    at = pl.ds(pl.multiple_of((first + j) * LANES, LANES), LANES)
                    clear, total, colours = state[j]
                    colours = [colours[c] + clear * mid[c, :, at] for c in range(3)]
                    state[j] = (clear * mid[3, :, at], total, colours)
        return state

    over_columns(outs, me, inner, column)


def full_kernel(absorb, inner, strip_of, strips, shear, footprint, vol, up, down, prev, nxt, *refs):
    edges, outs, (field, moved_v, moved_s) = refs[: -3 - inner], refs[-3 - inner : -3], refs[-3:]
    slices = vol.shape[0]
    me = lax.axis_index("depth")
    flip = shear[0] > shear[shear.shape[0] - 1]
    clear_edges(moved_v, moved_s)
    centre = [(s + 1, s, s) for s in range(slices)]
    set_edges(field, centre, strip_of(pl.program_id(0)), strips, up, down, edges)

    def widen_step(s, carry):
        widen(field, s + 1, vol[s], 8)
        return carry

    lax.fori_loop(0, slices, widen_step, 0)
    widen(field, 0, prev[...], 8)
    widen(field, slices + 1, nxt[...], 8)

    def shade_step(i, carry):
        narrow = lambda t: vol[i, :, t * LANES : (t + 1) * LANES]
        shade_slice(field, moved_v, moved_s, i + 1, shear[me * slices + i], i, 0, narrow)
        return carry

    lax.fori_loop(0, slices, shade_step, 0)

    def column(first, count):
        rate = rates(absorb, footprint, first, count)
        state = fresh(count)
        for step in range(slices):
            i = jnp.where(flip, slices - 1 - step, step)
            shift = shear[me * slices + i]
            state = blend(state, moved_v, moved_s, i, shift, first, count, rate)
        return state

    over_columns(outs, me, inner, column)


def encode(x):
    x = jnp.maximum(x, 1e-30)
    code = (x * lax.rsqrt(x) * 65535.0 + 0.5).astype(jnp.int32) - 32768
    return code.astype(LINK)


def decode(code):
    root = (code.astype(jnp.int32) + 32768).astype(jnp.float32) * (1.0 / 65535.0)
    return root * root


def over(pieces):
    image = pieces[0]
    for piece in pieces[1:]:
        clear = 1.0 - image[3]
        image = [image[c] + clear * piece[c] for c in range(4)]
    return image


def ordered(count, mine, flip, body):
    cases = {}
    for position in range(count):
        for turned in (False, True):
            order = tuple((position - p) % count for p in range(count))
            cases.setdefault(order[::-1] if turned else order, []).append((position, turned))
    for order, where in cases.items():
        chosen = functools.reduce(
            jnp.logical_or, [(mine == position) & (flip == turned) for position, turned in where]
        )
        pl.when(chosen)(functools.partial(body, order))


def group_kernel(inner, shear, *refs):
    sources, outs = refs[:inner], refs[inner:]
    me = lax.axis_index("depth")
    flip = shear[0] > shear[shear.shape[0] - 1]
    groups = len(outs)

    def body(order):
        for k in range(groups):
            target = lax.rem(lax.div(me, inner) + k, groups)
            pieces = [
                [sources[shift][target, c].astype(jnp.float32) for c in range(4)]
                for shift in order
            ]
            for c, value in enumerate(over(pieces)):
                outs[k][c] = encode(value)

    ordered(inner, lax.rem(me, inner), flip, body)


def frame_kernel(inner, aliased, shear, *refs):
    sources, out = refs[:-1], refs[-1]
    if aliased:
        sources = sources[:-1]
    me = lax.axis_index("depth")
    flip = shear[0] > shear[shear.shape[0] - 1]

    def body(order):
        pieces = [[decode(sources[shift][c]) for c in range(4)] for shift in order]
        for c, value in enumerate(over(pieces)):
            out[c] = value

    ordered(len(sources), lax.div(me, inner), flip, body)


def shards(volume, shear, footprint):
    slices, rows, ny = volume.shape
    bricks = lax.axis_size("depth")
    crosswise = lax.axis_size("tile")
    absorb = 2.0 / (slices * bricks)
    inner = 1
    while 4 * inner * inner <= bricks:
        inner *= 2
    groups = bricks // inner
    width = ny // bricks
    tiles = ny // LANES
    strips = rows // ROWS

    def line(length):
        return [(i, i + 1) for i in range(length - 1)], [(i + 1, i) for i in range(length - 1)]

    depth_up, depth_down = line(bricks)
    row_up, row_down = line(crosswise)

    parts = [(1, strips - 2)] if strips > 2 else []
    parts += [(s, 1) for s in sorted({0, strips - 1})]

    prev = lax.ppermute(volume[slices - 1], "depth", depth_up)
    nxt = lax.ppermute(volume[0], "depth", depth_down)
    above = lax.ppermute(volume[:, rows - 1, :], "tile", row_up)
    below = lax.ppermute(volume[:, 0, :], "tile", row_down)

    vmem = pl.BlockSpec(memory_space=pltpu.VMEM)
    smem = pl.BlockSpec(memory_space=pltpu.SMEM)
    anywhere = pl.BlockSpec(memory_space=pl.ANY)
    moved = lambda n: pltpu.VMEM((n, tiles + 2, ROWS, LANES), jnp.float32)
    field = lambda n: pltpu.VMEM((n, tiles, ROWS + 20, LANES), jnp.float32)
    received = []
    for part in parts:
        first, count = part
        chunk = count * ROWS
        strip_of = lambda i, first=first: first + i
        flat = pl.BlockSpec((ROWS, ny), lambda i, first=first: (first + i, 0))
        edges = [above, below] if first == 0 or first + count == strips else []

        def slab(size, s, move=0, strip_of=strip_of):
            if move == 0:
                return pl.BlockSpec((size, ROWS, ny), lambda i: (s, strip_of(i), 0))
            offset = -1 if move < 0 else ROWS // 8

            def index(i):
                return s, jnp.clip(strip_of(i) * (ROWS // 8) + offset, 0, rows // 8 - 1), 0

            return pl.BlockSpec((size, 8, ny), index)

        def cost(per, chunk=chunk):
            return pl.CostEstimate(
                flops=per * chunk * ny, bytes_accessed=chunk * ny * 32, transcendentals=0
            )

        side_shape = [jax.ShapeDtypeStruct((groups, 4, chunk, width), jnp.bfloat16)] * inner
        side_spec = [pl.BlockSpec((groups, 4, ROWS, width), lambda i: (0, 0, i, 0))] * inner
        whole = [slab(slices, 0), slab(slices, 0, -1), slab(slices, 0, 1)]
        if not edges:
            middle = pl.BlockSpec((4, ROWS, ny), lambda i: (0, i, 0))
            mid = pl.pallas_call(
                functools.partial(inner_kernel, absorb, strip_of, strips),
                out_shape=jax.ShapeDtypeStruct((4, chunk, ny), jnp.float32),
                grid=(count,),
                in_specs=[smem, smem] + whole + [vmem] * len(edges),
                out_specs=middle,
                scratch_shapes=[field(slices), moved(slices - 2), moved(slices - 2)],
                cost_estimate=cost(800),
                compiler_params=params(INNER_MIB),
                name="inner",
            )(shear, footprint, *[volume] * 3, *edges)
            sides = pl.pallas_call(
                functools.partial(outer_kernel, absorb, inner, strip_of, strips),
                out_shape=side_shape,
                grid=(count,),
                in_specs=[smem, smem, slab(2, 0), slab(2, slices // 2 - 1)]
                + [slab(1, 0, -1), slab(1, 0, 1), slab(1, slices - 1, -1), slab(1, slices - 1, 1)]
                + [flat, flat, middle]
                + [vmem] * len(edges),
                out_specs=side_spec,
                scratch_shapes=[field(6), moved(2), moved(2)],
                cost_estimate=cost(400),
                compiler_params=params(OUTER_MIB),
                name="outer",
            )(shear, footprint, *[volume] * 6, prev, nxt, mid, *edges)
        else:
            sides = pl.pallas_call(
                functools.partial(full_kernel, absorb, inner, strip_of, strips),
                out_shape=side_shape,
                grid=(count,),
                in_specs=[smem, smem] + whole + [flat, flat] + [vmem] * len(edges),
                out_specs=side_spec,
                scratch_shapes=[field(slices + 2), moved(slices), moved(slices)],
                cost_estimate=cost(1100),
                compiler_params=params(OUTER_MIB),
                name="full",
            )(shear, footprint, *[volume] * 3, prev, nxt, *edges)
        sides = list(sides)
        for k in range(1, inner):
            pairs = [
                (g * inner + x, g * inner + (x + k) % inner)
                for g in range(groups)
                for x in range(inner)
            ]
            sides[k] = lax.ppermute(sides[k], "depth", pairs)
        received.append(sides)

    frame = None
    for (first, count), sides in zip(parts, received):
        chunk = count * ROWS
        pieces = pl.pallas_call(
            functools.partial(group_kernel, inner),
            out_shape=[jax.ShapeDtypeStruct((4, chunk, width), LINK)] * groups,
            grid=(count,),
            in_specs=[smem]
            + [pl.BlockSpec((groups, 4, ROWS, width), lambda i: (0, 0, i, 0))] * inner,
            out_specs=[pl.BlockSpec((4, ROWS, width), lambda i: (0, i, 0))] * groups,
            cost_estimate=pl.CostEstimate(
                flops=20 * chunk * ny, bytes_accessed=2 << 20, transcendentals=0
            ),
            compiler_params=params(16),
            name="group",
        )(shear, *sides)
        pieces = list(pieces)
        for k in range(1, groups):
            pairs = [
                (g * inner + x, (g + k) % groups * inner + x)
                for g in range(groups)
                for x in range(inner)
            ]
            pieces[k] = lax.ppermute(pieces[k], "depth", pairs)
        frame = pl.pallas_call(
            functools.partial(frame_kernel, inner, frame is not None),
            out_shape=jax.ShapeDtypeStruct((4, rows, width), jnp.float32),
            grid=(count,),
            in_specs=[smem]
            + [pl.BlockSpec((4, ROWS, width), lambda i: (0, i, 0))] * groups
            + [anywhere] * (frame is not None),
            out_specs=pl.BlockSpec(
                (4, ROWS, width), lambda i, first=first: (0, first + i, 0)
            ),
            input_output_aliases={} if frame is None else {1 + groups: 0},
            cost_estimate=pl.CostEstimate(
                flops=20 * chunk * width, bytes_accessed=2 << 20, transcendentals=0
            ),
            compiler_params=params(16),
            name="frame",
        )(shear, *pieces, *([] if frame is None else [frame]))
    return frame


def solution(mesh):
    placed = (P("depth", "tile", None), P(), P("depth", None))
    return jax.shard_map(
        shards, mesh=mesh, in_specs=placed, out_specs=P(None, "tile", "depth"), check_vma=False
    )
```

```python
import functools

import jax
import jax.numpy as jnp
from jax import lax
from jax.experimental import pallas as pl
from jax.experimental.pallas import tpu as pltpu
from jax.sharding import PartitionSpec as P


LANES = 128
ROWS = 16
LOG2E = 1.4426950408889634
LINK = jnp.int16
INNER_MIB = 48
OUTER_MIB = 24


def params(mib):
    return pltpu.CompilerParams(vmem_limit_bytes=mib << 20)


def difference(across, steps, narrow):
    tiles = across.shape[0]
    none = jnp.zeros((ROWS, LANES), jnp.bfloat16)
    line = [none] + [narrow(t) for t in range(tiles)] + [none]
    windows = [jnp.concatenate(line[t : t + 4], axis=1) for t in range(0, tiles, 2)]
    found = jnp.dot(
        jnp.concatenate(windows, axis=0), steps[...], preferred_element_type=jnp.float32
    )
    for t in range(tiles):
        row, column = t // 2 * ROWS, t % 2 * LANES
        across[t] = found[row : row + ROWS, column : column + LANES]


def shade(field, moved_v, moved_s, across, where, shift, base, narrow):
    turn = jnp.where(shift < 0, shift + LANES, shift)
    here, up, down = pl.ds(8, ROWS), pl.ds(7, ROWS), pl.ds(9, ROWS)
    for t in range(field.shape[1]):
        dy = across[t]
        dz = field[where + 1, t, here, :] - field[where - 1, t, here, :]
        dx = field[where, t, down, :] - field[where, t, up, :]
        squares = (dx * dx + dy * dy) + (dz * dz + 4.0)
        along = (0.35 * 0.48) * dx + (0.35 * 0.6) * dy + (0.35 * 0.64) * dz
        half = 0.15 + jnp.abs(along) * lax.rsqrt(squares)
        moved_s[base, t + 1] = pltpu.roll(half, turn, 1)
        moved_v[base, t + 1] = pltpu.roll(narrow(t), turn, 1).astype(jnp.float32)


def shade_all(field, moved_v, moved_s, across, steps, count, where, shift, narrow):
    even, odd = across
    difference(even, steps, narrow(0))

    def pair_step(pair, carry):
        i = 2 * pair
        difference(odd, steps, narrow(i + 1))
        shade(field, moved_v, moved_s, even, where(i), shift(i), i, narrow(i))
        difference(even, steps, narrow(jnp.minimum(i + 2, count - 1)))
        shade(field, moved_v, moved_s, odd, where(i + 1), shift(i + 1), i + 1, narrow(i + 1))
        return carry

    lax.fori_loop(0, count // 2, pair_step, 0)


def blend(state, moved_v, moved_s, index, shift, first, count, rate):
    lane = lax.broadcasted_iota(jnp.int32, (ROWS, LANES), 1)
    turn = jnp.where(shift < 0, shift + LANES, shift)
    start = first + jnp.where(shift < 0, 1, 0)
    keep = lane < turn
    values = [moved_v[index, start + j] for j in range(count + 1)]
    shades = [moved_s[index, start + j] for j in range(count + 1)]
    result = []
    for j in range(count):
        clear, total, colours = state[j]
        v = jnp.where(keep, values[j], values[j + 1])
        half = jnp.where(keep, shades[j], shades[j + 1])
        left = clear * jnp.exp2(v * v * rate[j])
        weight = (clear - left) * half
        arguments = (0.6 * v + 0.1, -0.4 * v, 0.25 * v - 0.15)
        colours = [colours[c] + weight * jnp.tanh(arguments[c]) for c in range(3)]
        result.append((left, total + weight, colours))
    return result


def rates(absorb, footprint, first, count):
    lane = lax.broadcasted_iota(jnp.int32, (ROWS, LANES), 1)
    found = []
    for j in range(count):
        column = lane + (first + j) * LANES
        inside = (column >= footprint[0, 0]) & (column < footprint[0, 1])
        found.append(jnp.where(inside, -absorb * LOG2E, 0.0))
    return found


def fresh(count):
    zero = jnp.zeros((ROWS, LANES), jnp.float32)
    return [(zero + 1.0, zero, [zero] * 3) for _ in range(count)]


def widen(field, index, line, place):
    line = line.astype(jnp.float32)
    for t in range(field.shape[1]):
        field[index, t, place : place + line.shape[0], :] = line[:, t * LANES : (t + 1) * LANES]


def set_row(field, index, place, line):
    for t in range(field.shape[1]):
        field[index, t, place : place + 1, :] = line[:, t * LANES : (t + 1) * LANES]


def set_edges(field, slices, strip, strips, up, down, edges):
    for index, block, _ in slices:
        widen(field, index, up[block], 0)
        widen(field, index, down[block], 8 + ROWS)
    if not edges:
        return
    for edge, last, place in ((edges[0], 0, 7), (edges[1], strips - 1, 8 + ROWS)):

        @pl.when(strip == last)
        def _(edge=edge, place=place):
            line = edge[...].astype(jnp.float32)
            for index, _, s in slices:
                set_row(field, index, place, line[s : s + 1])


def prepare(moved_v, moved_s, steps):
    @pl.when(pl.program_id(0) == 0)
    def _():
        at = lax.broadcasted_iota(jnp.int32, steps.shape, 0)
        to = lax.broadcasted_iota(jnp.int32, steps.shape, 1) + LANES
        ahead = jnp.where(at == to + 1, 1.0, 0.0)
        steps[...] = jnp.where(at == to - 1, -1.0, ahead).astype(jnp.bfloat16)
        tiles = moved_v.shape[1] - 2
        zero = jnp.zeros((moved_v.shape[0], ROWS, LANES), jnp.float32)
        for t in (0, tiles + 1):
            moved_v[:, t] = zero
            moved_s[:, t] = zero


def emit(state, outs, slot, group, part, count):
    for j in range(count):
        at = pl.ds(pl.multiple_of((part * count + j) * LANES, LANES), LANES)
        clear, total, colours = state[j]
        for c in range(3):
            outs[slot][group, c, :, at] = (total + colours[c]).astype(jnp.bfloat16)
        outs[slot][group, 3, :, at] = (1.0 - clear).astype(jnp.bfloat16)


def over_columns(outs, me, inner, body):
    groups, _, _, width = outs[0].shape
    per = width // LANES
    count = min(2, per)
    for slot in range(inner):
        column = lax.rem(lax.rem(me, inner) + slot, inner)

        def column_step(i, carry, slot=slot, column=column):
            group, part = i // (per // count), lax.rem(i, per // count)
            first = (group * inner + column) * per + part * count
            emit(body(first, count), outs, slot, group, part, count)
            return carry

        lax.fori_loop(0, groups * (per // count), column_step, 0)


def inner_kernel(absorb, strip_of, strips, shear, footprint, vol, up, down, *refs):
    edges, (out, field, moved_v, moved_s, *across, steps) = refs[:-7], refs[-7:]
    slices, _, ny = vol.shape
    me = lax.axis_index("depth")
    flip = shear[0] > shear[shear.shape[0] - 1]
    prepare(moved_v, moved_s, steps)
    centre = [(s, s, s) for s in range(1, slices - 1)]
    set_edges(field, centre, strip_of(pl.program_id(0)), strips, up, down, edges)

    def widen_step(s, carry):
        widen(field, s, vol[s], 8)
        return carry

    lax.fori_loop(0, slices, widen_step, 0)

    shade_all(
        field,
        moved_v,
        moved_s,
        across,
        steps,
        slices - 2,
        lambda i: i + 1,
        lambda i: shear[me * slices + i + 1],
        lambda i: lambda t: vol[i + 1, :, t * LANES : (t + 1) * LANES],
    )

    def column_step(pair, carry):
        first = 2 * pair
        rate = rates(absorb, footprint, first, 2)
        state = fresh(2)
        for step in range(slices - 2):
            i = jnp.where(flip, slices - 3 - step, step)
            shift = shear[me * slices + i + 1]
            state = blend(state, moved_v, moved_s, i, shift, first, 2, rate)
        for j in range(2):
            at = pl.ds(pl.multiple_of((first + j) * LANES, LANES), LANES)
            clear, total, colours = state[j]
            for c in range(3):
                out[c, :, at] = total + colours[c]
            out[3, :, at] = clear
        return carry

    lax.fori_loop(0, ny // LANES // 2, column_step, 0)


def outer_kernel(absorb, inner, strip_of, strips, shear, footprint, *refs):
    front, back, front_up, front_down, back_up, back_down, prev, nxt, mid = refs[:9]
    edges, outs, (field, moved_v, moved_s, *across, steps) = refs[9 : -6 - inner], refs[-6 - inner : -6], refs[-6:]
    me = lax.axis_index("depth")
    flip = shear[0] > shear[shear.shape[0] - 1]
    slices = shear.shape[0] // lax.axis_size("depth")
    strip = strip_of(pl.program_id(0))
    prepare(moved_v, moved_s, steps)
    set_edges(field, [(1, 0, 0)], strip, strips, front_up, front_down, edges)
    set_edges(field, [(4, 0, slices - 1)], strip, strips, back_up, back_down, edges)
    for index, line in enumerate((prev, front.at[0], front.at[1], back.at[0], back.at[1], nxt)):
        widen(field, index, line[...], 8)
    ends = [front.at[0], back.at[1]]
    narrow = lambda i: lambda t: ends[i][:, t * LANES : (t + 1) * LANES]
    for i in range(2):
        difference(across[i], steps, narrow(i))
    for i in range(2):
        shift = shear[me * slices + i * (slices - 1)]
        shade(field, moved_v, moved_s, across[i], 1 + 3 * i, shift, i, narrow(i))

    def column(first, count):
        rate = rates(absorb, footprint, first, count)
        state = fresh(count)
        for step in range(2):
            i = jnp.where(flip, 1 - step, step)
            shift = shear[me * slices + i * (slices - 1)]
            state = blend(state, moved_v, moved_s, i, shift, first, count, rate)
            if step == 0:
                for j in range(count):
                    at = pl.ds(pl.multiple_of((first + j) * LANES, LANES), LANES)
                    clear, total, colours = state[j]
                    colours = [colours[c] + clear * mid[c, :, at] for c in range(3)]
                    state[j] = (clear * mid[3, :, at], total, colours)
        return state

    over_columns(outs, me, inner, column)


def encode(x):
    x = jnp.maximum(x, 1e-30)
    code = (x * lax.rsqrt(x) * 65535.0 + 0.5).astype(jnp.int32) - 32768
    return code.astype(LINK)


def decode(code):
    root = (code.astype(jnp.int32) + 32768).astype(jnp.float32) * (1.0 / 65535.0)
    return root * root


def over(pieces):
    image = pieces[0]
    for piece in pieces[1:]:
        clear = 1.0 - image[3]
        image = [image[c] + clear * piece[c] for c in range(4)]
    return image


def ordered(count, mine, flip, body):
    cases = {}
    for position in range(count):
        for turned in (False, True):
            order = tuple((position - p) % count for p in range(count))
            cases.setdefault(order[::-1] if turned else order, []).append((position, turned))
    for order, where in cases.items():
        chosen = functools.reduce(
            jnp.logical_or, [(mine == position) & (flip == turned) for position, turned in where]
        )
        pl.when(chosen)(functools.partial(body, order))


def group_kernel(inner, shear, *refs):
    sources, outs = refs[:inner], refs[inner:]
    me = lax.axis_index("depth")
    flip = shear[0] > shear[shear.shape[0] - 1]
    groups = len(outs)

    def body(order):
        for k in range(groups):
            target = lax.rem(lax.div(me, inner) + k, groups)
            pieces = [
                [sources[shift][target, c].astype(jnp.float32) for c in range(4)]
                for shift in order
            ]
            for c, value in enumerate(over(pieces)):
                outs[k][c] = encode(value)

    ordered(inner, lax.rem(me, inner), flip, body)


def frame_kernel(inner, aliased, shear, *refs):
    sources, out = refs[:-1], refs[-1]
    if aliased:
        sources = sources[:-1]
    me = lax.axis_index("depth")
    flip = shear[0] > shear[shear.shape[0] - 1]

    def body(order):
        pieces = [[decode(sources[shift][c]) for c in range(4)] for shift in order]
        for c, value in enumerate(over(pieces)):
            out[c] = value

    ordered(len(sources), lax.div(me, inner), flip, body)


def shards(volume, shear, footprint):
    slices, rows, ny = volume.shape
    bricks = lax.axis_size("depth")
    crosswise = lax.axis_size("tile")
    absorb = 2.0 / (slices * bricks)
    inner = 1
    while 4 * inner * inner <= bricks:
        inner *= 2
    groups = bricks // inner
    width = ny // bricks
    tiles = ny // LANES
    strips = rows // ROWS

    def line(length):
        return [(i, i + 1) for i in range(length - 1)], [(i + 1, i) for i in range(length - 1)]

    depth_up, depth_down = line(bricks)
    row_up, row_down = line(crosswise)

    batches = [(1, 1, strips - 2)] if strips > 2 else []
    batches += [(0, max(strips - 1, 1), min(strips, 2))]
    parts = [(1, strips - 2, 0, 0)] if strips > 2 else []
    parts += [(s, 1, len(batches) - 1, i) for i, s in enumerate(sorted({0, strips - 1}))]

    prev = lax.ppermute(volume[slices - 1], "depth", depth_up)
    nxt = lax.ppermute(volume[0], "depth", depth_down)
    above = lax.ppermute(volume[:, rows - 1, :], "tile", row_up)
    below = lax.ppermute(volume[:, 0, :], "tile", row_down)

    vmem = pl.BlockSpec(memory_space=pltpu.VMEM)
    smem = pl.BlockSpec(memory_space=pltpu.SMEM)
    anywhere = pl.BlockSpec(memory_space=pl.ANY)
    moved = lambda n: pltpu.VMEM((n, tiles + 2, ROWS, LANES), jnp.float32)
    field = lambda n: pltpu.VMEM((n, tiles, ROWS + 20, LANES), jnp.float32)
    across = pltpu.VMEM((tiles, ROWS, LANES), jnp.float32)
    steps = pltpu.VMEM((4 * LANES, 2 * LANES), jnp.bfloat16)

    def slab(strip_of, size, s, move=0):
        if move == 0:
            return pl.BlockSpec((size, ROWS, ny), lambda i: (s, strip_of(i), 0))
        offset = -1 if move < 0 else ROWS // 8

        def index(i):
            return s, jnp.clip(strip_of(i) * (ROWS // 8) + offset, 0, rows // 8 - 1), 0

        return pl.BlockSpec((size, 8, ny), index)

    def cost(chunk, per):
        return pl.CostEstimate(
            flops=per * chunk * ny, bytes_accessed=chunk * ny * 32, transcendentals=0
        )

    mids = []
    for first, step, count in batches:
        strip_of = lambda i, first=first, step=step: first + step * i
        edges = [above, below] if first == 0 else []
        mid = pl.pallas_call(
            functools.partial(inner_kernel, absorb, strip_of, strips),
            out_shape=jax.ShapeDtypeStruct((4, count * ROWS, ny), jnp.float32),
            grid=(count,),
            in_specs=[smem, smem]
            + [slab(strip_of, slices, 0, move) for move in (0, -1, 1)]
            + [vmem] * len(edges),
            out_specs=pl.BlockSpec((4, ROWS, ny), lambda i: (0, i, 0)),
            scratch_shapes=[field(slices), moved(slices - 2), moved(slices - 2)]
            + [across, across, steps],
            cost_estimate=cost(count * ROWS, 800),
            compiler_params=params(INNER_MIB),
            name="inner",
        )(shear, footprint, *[volume] * 3, *edges)
        mids.append(mid)

    received = []
    for first, count, batch, place in parts:
        chunk = count * ROWS
        strip_of = lambda i, first=first: first + i
        edges = [above, below] if first == 0 or first + count == strips else []
        flat = pl.BlockSpec((ROWS, ny), lambda i, first=first: (first + i, 0))
        ends = [(2, 0, 0), (2, slices // 2 - 1, 0)]
        ends += [(1, s, move) for s in (0, slices - 1) for move in (-1, 1)]
        sides = pl.pallas_call(
            functools.partial(outer_kernel, absorb, inner, strip_of, strips),
            out_shape=[jax.ShapeDtypeStruct((groups, 4, chunk, width), jnp.bfloat16)] * inner,
            grid=(count,),
            in_specs=[smem, smem]
            + [slab(strip_of, *end) for end in ends]
            + [flat, flat]
            + [pl.BlockSpec((4, ROWS, ny), lambda i, place=place: (0, place + i, 0))]
            + [vmem] * len(edges),
            out_specs=[pl.BlockSpec((groups, 4, ROWS, width), lambda i: (0, 0, i, 0))] * inner,
            scratch_shapes=[field(6), moved(2), moved(2), across, across, steps],
            cost_estimate=cost(chunk, 400),
            compiler_params=params(OUTER_MIB),
            name="outer",
        )(shear, footprint, *[volume] * 6, prev, nxt, mids[batch], *edges)
        sides = list(sides)
        for k in range(1, inner):
            pairs = [
                (g * inner + x, g * inner + (x + k) % inner)
                for g in range(groups)
                for x in range(inner)
            ]
            sides[k] = lax.ppermute(sides[k], "depth", pairs)
        received.append(sides)

    frame = None
    for (first, count, _, _), sides in zip(parts, received):
        chunk = count * ROWS
        pieces = pl.pallas_call(
            functools.partial(group_kernel, inner),
            out_shape=[jax.ShapeDtypeStruct((4, chunk, width), LINK)] * groups,
            grid=(count,),
            in_specs=[smem]
            + [pl.BlockSpec((groups, 4, ROWS, width), lambda i: (0, 0, i, 0))] * inner,
            out_specs=[pl.BlockSpec((4, ROWS, width), lambda i: (0, i, 0))] * groups,
            cost_estimate=pl.CostEstimate(
                flops=20 * chunk * ny, bytes_accessed=2 << 20, transcendentals=0
            ),
            compiler_params=params(16),
            name="group",
        )(shear, *sides)
        pieces = list(pieces)
        for k in range(1, groups):
            pairs = [
                (g * inner + x, (g + k) % groups * inner + x)
                for g in range(groups)
                for x in range(inner)
            ]
            pieces[k] = lax.ppermute(pieces[k], "depth", pairs)
        frame = pl.pallas_call(
            functools.partial(frame_kernel, inner, frame is not None),
            out_shape=jax.ShapeDtypeStruct((4, rows, width), jnp.float32),
            grid=(count,),
            in_specs=[smem]
            + [pl.BlockSpec((4, ROWS, width), lambda i: (0, i, 0))] * groups
            + [anywhere] * (frame is not None),
            out_specs=pl.BlockSpec(
                (4, ROWS, width), lambda i, first=first: (0, first + i, 0)
            ),
            input_output_aliases={} if frame is None else {1 + groups: 0},
            cost_estimate=pl.CostEstimate(
                flops=20 * chunk * width, bytes_accessed=2 << 20, transcendentals=0
            ),
            compiler_params=params(16),
            name="frame",
        )(shear, *pieces, *([] if frame is None else [frame]))
    return frame


def solution(mesh):
    placed = (P("depth", "tile", None), P(), P("depth", None))
    return jax.shard_map(
        shards, mesh=mesh, in_specs=placed, out_specs=P(None, "tile", "depth"), check_vma=False
    )
```

```python
import functools

import jax
import jax.numpy as jnp
from jax import lax
from jax.experimental import pallas as pl
from jax.experimental.pallas import tpu as pltpu
from jax.sharding import PartitionSpec as P


LANES = 128
ROWS = 16
LOG2E = 1.4426950408889634
LINK = jnp.int16
INNER_MIB = 48
OUTER_MIB = 24


def params(mib):
    return pltpu.CompilerParams(vmem_limit_bytes=mib << 20)


def difference(across, steps, narrow):
    tiles = across.shape[0]
    none = jnp.zeros((ROWS, LANES), jnp.bfloat16)
    line = [none] + [narrow(t) for t in range(tiles)] + [none]
    windows = [jnp.concatenate(line[t : t + 4], axis=1) for t in range(0, tiles, 2)]
    found = jnp.dot(
        jnp.concatenate(windows, axis=0), steps[...], preferred_element_type=jnp.float32
    )
    for t in range(tiles):
        row, column = t // 2 * ROWS, t % 2 * LANES
        across[t] = found[row : row + ROWS, column : column + LANES]


def shade(field, moved_v, moved_s, across, where, shift, base, narrow):
    turn = jnp.where(shift < 0, shift + LANES, shift)
    here, up, down = pl.ds(8, ROWS), pl.ds(7, ROWS), pl.ds(9, ROWS)
    for t in range(field.shape[1]):
        dy = across[t]
        dz = field[where + 1, t, here, :] - field[where - 1, t, here, :]
        dx = field[where, t, down, :] - field[where, t, up, :]
        squares = (dx * dx + dy * dy) + (dz * dz + 4.0)
        along = (0.35 * 0.48) * dx + (0.35 * 0.6) * dy + (0.35 * 0.64) * dz
        half = 0.15 + jnp.abs(along) * lax.rsqrt(squares)
        moved_s[base, t + 1] = pltpu.roll(half, turn, 1)
        moved_v[base, t + 1] = pltpu.roll(narrow(t), turn, 1).astype(jnp.float32)


def shade_all(field, moved_v, moved_s, across, steps, count, where, shift, narrow):
    even, odd = across
    difference(even, steps, narrow(0))

    def pair_step(pair, carry):
        i = 2 * pair
        difference(odd, steps, narrow(i + 1))
        shade(field, moved_v, moved_s, even, where(i), shift(i), i, narrow(i))
        difference(even, steps, narrow(jnp.minimum(i + 2, count - 1)))
        shade(field, moved_v, moved_s, odd, where(i + 1), shift(i + 1), i + 1, narrow(i + 1))
        return carry

    lax.fori_loop(0, count // 2, pair_step, 0)


def blend(state, moved_v, moved_s, index, shift, first, count, rate):
    lane = lax.broadcasted_iota(jnp.int32, (ROWS, LANES), 1)
    turn = jnp.where(shift < 0, shift + LANES, shift)
    start = first + jnp.where(shift < 0, 1, 0)
    keep = lane < turn
    values = [moved_v[index, start + j] for j in range(count + 1)]
    shades = [moved_s[index, start + j] for j in range(count + 1)]
    result = []
    for j in range(count):
        clear, total, colours = state[j]
        v = jnp.where(keep, values[j], values[j + 1])
        half = jnp.where(keep, shades[j], shades[j + 1])
        left = clear * jnp.exp2(v * v * rate[j])
        weight = (clear - left) * half
        arguments = (0.6 * v + 0.1, -0.4 * v, 0.25 * v - 0.15)
        colours = [colours[c] + weight * jnp.tanh(arguments[c]) for c in range(3)]
        result.append((left, total + weight, colours))
    return result


def rates(absorb, footprint, first, count):
    lane = lax.broadcasted_iota(jnp.int32, (ROWS, LANES), 1)
    found = []
    for j in range(count):
        column = lane + (first + j) * LANES
        inside = (column >= footprint[0, 0]) & (column < footprint[0, 1])
        found.append(jnp.where(inside, -absorb * LOG2E, 0.0))
    return found


def fresh(count):
    zero = jnp.zeros((ROWS, LANES), jnp.float32)
    return [(zero + 1.0, zero, [zero] * 3) for _ in range(count)]


def widen(field, index, line, place):
    line = line.astype(jnp.float32)
    for t in range(field.shape[1]):
        field[index, t, place : place + line.shape[0], :] = line[:, t * LANES : (t + 1) * LANES]


def set_row(field, index, place, line):
    for t in range(field.shape[1]):
        field[index, t, place : place + 1, :] = line[:, t * LANES : (t + 1) * LANES]


def set_edges(field, slices, strip, strips, up, down, edges):
    for index, block, _ in slices:
        widen(field, index, up[block], 0)
        widen(field, index, down[block], 8 + ROWS)
    if not edges:
        return
    for edge, last, place in ((edges[0], 0, 7), (edges[1], strips - 1, 8 + ROWS)):

        @pl.when(strip == last)
        def _(edge=edge, place=place):
            line = edge[...].astype(jnp.float32)
            for index, _, s in slices:
                set_row(field, index, place, line[s : s + 1])


def prepare(moved_v, moved_s, steps):
    @pl.when(pl.program_id(0) == 0)
    def _():
        at = lax.broadcasted_iota(jnp.int32, steps.shape, 0)
        to = lax.broadcasted_iota(jnp.int32, steps.shape, 1) + LANES
        ahead = jnp.where(at == to + 1, 1.0, 0.0)
        steps[...] = jnp.where(at == to - 1, -1.0, ahead).astype(jnp.bfloat16)
        tiles = moved_v.shape[1] - 2
        zero = jnp.zeros((moved_v.shape[0], ROWS, LANES), jnp.float32)
        for t in (0, tiles + 1):
            moved_v[:, t] = zero
            moved_s[:, t] = zero


def emit(state, outs, slot, group, part, count):
    for j in range(count):
        at = pl.ds(pl.multiple_of((part * count + j) * LANES, LANES), LANES)
        clear, total, colours = state[j]
        for c in range(3):
            outs[slot][group, c, :, at] = (total + colours[c]).astype(jnp.bfloat16)
        outs[slot][group, 3, :, at] = (1.0 - clear).astype(jnp.bfloat16)


def over_columns(outs, me, inner, body):
    groups, _, _, width = outs[0].shape
    per = width // LANES
    count = min(2, per)
    for slot in range(inner):
        column = lax.rem(lax.rem(me, inner) + slot, inner)

        def column_step(i, carry, slot=slot, column=column):
            group, part = i // (per // count), lax.rem(i, per // count)
            first = (group * inner + column) * per + part * count
            emit(body(first, count), outs, slot, group, part, count)
            return carry

        lax.fori_loop(0, groups * (per // count), column_step, 0)


def inner_kernel(absorb, strip_of, strips, shear, footprint, vol, up, down, *refs):
    edges, (out, field, moved_v, moved_s, *across, steps) = refs[:-7], refs[-7:]
    slices, _, ny = vol.shape
    me = lax.axis_index("depth")
    flip = shear[0] > shear[shear.shape[0] - 1]
    prepare(moved_v, moved_s, steps)
    centre = [(s, s, s) for s in range(1, slices - 1)]
    set_edges(field, centre, strip_of(pl.program_id(0)), strips, up, down, edges)

    def widen_step(s, carry):
        widen(field, s, vol[s], 8)
        return carry

    lax.fori_loop(0, slices, widen_step, 0)

    shade_all(
        field,
        moved_v,
        moved_s,
        across,
        steps,
        slices - 2,
        lambda i: i + 1,
        lambda i: shear[me * slices + i + 1],
        lambda i: lambda t: vol[i + 1, :, t * LANES : (t + 1) * LANES],
    )

    def column_step(pair, carry):
        first = 2 * pair
        rate = rates(absorb, footprint, first, 2)
        state = fresh(2)
        for step in range(slices - 2):
            i = jnp.where(flip, slices - 3 - step, step)
            shift = shear[me * slices + i + 1]
            state = blend(state, moved_v, moved_s, i, shift, first, 2, rate)
        for j in range(2):
            at = pl.ds(pl.multiple_of((first + j) * LANES, LANES), LANES)
            clear, total, colours = state[j]
            for c in range(3):
                out[c, :, at] = total + colours[c]
            out[3, :, at] = clear
        return carry

    lax.fori_loop(0, ny // LANES // 2, column_step, 0)


def outer_kernel(absorb, inner, strip_of, strips, shear, footprint, *refs):
    front, back, front_up, front_down, back_up, back_down, prev, nxt, mid = refs[:9]
    edges, outs, (field, moved_v, moved_s, *across, steps) = refs[9 : -6 - inner], refs[-6 - inner : -6], refs[-6:]
    me = lax.axis_index("depth")
    flip = shear[0] > shear[shear.shape[0] - 1]
    slices = shear.shape[0] // lax.axis_size("depth")
    strip = strip_of(pl.program_id(0))
    prepare(moved_v, moved_s, steps)
    set_edges(field, [(1, 0, 0)], strip, strips, front_up, front_down, edges)
    set_edges(field, [(4, 0, slices - 1)], strip, strips, back_up, back_down, edges)
    for index, line in enumerate((prev, front.at[0], front.at[1], back.at[0], back.at[1], nxt)):
        widen(field, index, line[...], 8)
    ends = [front.at[0], back.at[1]]
    narrow = lambda i: lambda t: ends[i][:, t * LANES : (t + 1) * LANES]
    for i in range(2):
        difference(across[i], steps, narrow(i))
    for i in range(2):
        shift = shear[me * slices + i * (slices - 1)]
        shade(field, moved_v, moved_s, across[i], 1 + 3 * i, shift, i, narrow(i))

    def column(first, count):
        rate = rates(absorb, footprint, first, count)
        state = fresh(count)
        for step in range(2):
            i = jnp.where(flip, 1 - step, step)
            shift = shear[me * slices + i * (slices - 1)]
            state = blend(state, moved_v, moved_s, i, shift, first, count, rate)
            if step == 0:
                for j in range(count):
                    at = pl.ds(pl.multiple_of((first + j) * LANES, LANES), LANES)
                    clear, total, colours = state[j]
                    colours = [colours[c] + clear * mid[c, :, at] for c in range(3)]
                    state[j] = (clear * mid[3, :, at], total, colours)
        return state

    over_columns(outs, me, inner, column)


def encode(x):
    x = jnp.maximum(x, 1e-30)
    code = (x * lax.rsqrt(x) * 65535.0 + 0.5).astype(jnp.int32) - 32768
    return code.astype(LINK)


def decode(code):
    root = (code.astype(jnp.int32) + 32768).astype(jnp.float32) * (1.0 / 65535.0)
    return root * root


def over(pieces):
    image = pieces[0]
    for piece in pieces[1:]:
        clear = 1.0 - image[3]
        image = [image[c] + clear * piece[c] for c in range(4)]
    return image


def ordered(count, mine, flip, body):
    cases = {}
    for position in range(count):
        for turned in (False, True):
            order = tuple((position - p) % count for p in range(count))
            cases.setdefault(order[::-1] if turned else order, []).append((position, turned))
    for order, where in cases.items():
        chosen = functools.reduce(
            jnp.logical_or, [(mine == position) & (flip == turned) for position, turned in where]
        )
        pl.when(chosen)(functools.partial(body, order))


def group_kernel(inner, shear, *refs):
    sources, outs = refs[:inner], refs[inner:]
    me = lax.axis_index("depth")
    flip = shear[0] > shear[shear.shape[0] - 1]
    groups = len(outs)

    def body(order):
        def step(i, carry):
            at = pl.ds(pl.multiple_of(i * ROWS, ROWS), ROWS)
            for k in range(groups):
                target = lax.rem(lax.div(me, inner) + k, groups)
                pieces = [
                    [sources[shift][target, c, at, :].astype(jnp.float32) for c in range(4)]
                    for shift in order
                ]
                for c, value in enumerate(over(pieces)):
                    outs[k][c, at, :] = encode(value)
            return carry

        lax.fori_loop(0, outs[0].shape[1] // ROWS, step, 0)

    ordered(inner, lax.rem(me, inner), flip, body)


def frame_kernel(inner, aliased, shear, *refs):
    sources, out = refs[:-1], refs[-1]
    if aliased:
        sources = sources[:-1]
    me = lax.axis_index("depth")
    flip = shear[0] > shear[shear.shape[0] - 1]

    at = pl.ds(pl.multiple_of(pl.program_id(0) * ROWS, ROWS), ROWS)

    def body(order):
        pieces = [[decode(sources[shift][c, at, :]) for c in range(4)] for shift in order]
        for c, value in enumerate(over(pieces)):
            out[c] = value

    ordered(len(sources), lax.div(me, inner), flip, body)


def shards(volume, shear, footprint):
    slices, rows, ny = volume.shape
    bricks = lax.axis_size("depth")
    crosswise = lax.axis_size("tile")
    absorb = 2.0 / (slices * bricks)
    inner = 1
    while 4 * inner * inner <= bricks:
        inner *= 2
    groups = bricks // inner
    width = ny // bricks
    tiles = ny // LANES
    strips = rows // ROWS

    def line(length):
        return [(i, i + 1) for i in range(length - 1)], [(i + 1, i) for i in range(length - 1)]

    depth_up, depth_down = line(bricks)
    row_up, row_down = line(crosswise)

    batches = [(1, 1, strips - 2)] if strips > 2 else []
    batches += [(0, max(strips - 1, 1), min(strips, 2))]
    parts = [(*batches[-1], len(batches) - 1, 0)]
    if strips > 2:
        parts.insert(0, (1, 1, 1, 0, 0))
    if strips > 3:
        parts.append((2, 1, strips - 3, 0, 1))

    prev = lax.ppermute(volume[slices - 1], "depth", depth_up)
    nxt = lax.ppermute(volume[0], "depth", depth_down)
    above = lax.ppermute(volume[:, rows - 1, :], "tile", row_up)
    below = lax.ppermute(volume[:, 0, :], "tile", row_down)

    vmem = pl.BlockSpec(memory_space=pltpu.VMEM)
    smem = pl.BlockSpec(memory_space=pltpu.SMEM)
    anywhere = pl.BlockSpec(memory_space=pl.ANY)
    moved = lambda n: pltpu.VMEM((n, tiles + 2, ROWS, LANES), jnp.float32)
    field = lambda n: pltpu.VMEM((n, tiles, ROWS + 20, LANES), jnp.float32)
    across = pltpu.VMEM((tiles, ROWS, LANES), jnp.float32)
    steps = pltpu.VMEM((4 * LANES, 2 * LANES), jnp.bfloat16)

    def slab(strip_of, size, s, move=0):
        if move == 0:
            return pl.BlockSpec((size, ROWS, ny), lambda i: (s, strip_of(i), 0))
        offset = -1 if move < 0 else ROWS // 8

        def index(i):
            return s, jnp.clip(strip_of(i) * (ROWS // 8) + offset, 0, rows // 8 - 1), 0

        return pl.BlockSpec((size, 8, ny), index)

    def cost(chunk, per):
        return pl.CostEstimate(
            flops=per * chunk * ny, bytes_accessed=chunk * ny * 32, transcendentals=0
        )

    mids = []
    for first, step, count in batches:
        strip_of = lambda i, first=first, step=step: first + step * i
        edges = [above, below] if first == 0 else []
        mid = pl.pallas_call(
            functools.partial(inner_kernel, absorb, strip_of, strips),
            out_shape=jax.ShapeDtypeStruct((4, count * ROWS, ny), jnp.float32),
            grid=(count,),
            in_specs=[smem, smem]
            + [slab(strip_of, slices, 0, move) for move in (0, -1, 1)]
            + [vmem] * len(edges),
            out_specs=pl.BlockSpec((4, ROWS, ny), lambda i: (0, i, 0)),
            scratch_shapes=[field(slices), moved(slices - 2), moved(slices - 2)]
            + [across, across, steps],
            cost_estimate=cost(count * ROWS, 800),
            compiler_params=params(INNER_MIB),
            name="inner",
        )(shear, footprint, *[volume] * 3, *edges)
        mids.append(mid)

    received = []
    for first, step, count, batch, place in parts:
        chunk = count * ROWS
        strip_of = lambda i, first=first, step=step: first + step * i
        edges = [above, below] if first == 0 else []
        flat = pl.BlockSpec((ROWS, ny), lambda i, strip_of=strip_of: (strip_of(i), 0))
        ends = [(2, 0, 0), (2, slices // 2 - 1, 0)]
        ends += [(1, s, move) for s in (0, slices - 1) for move in (-1, 1)]
        sides = pl.pallas_call(
            functools.partial(outer_kernel, absorb, inner, strip_of, strips),
            out_shape=[jax.ShapeDtypeStruct((groups, 4, chunk, width), jnp.bfloat16)] * inner,
            grid=(count,),
            in_specs=[smem, smem]
            + [slab(strip_of, *end) for end in ends]
            + [flat, flat]
            + [pl.BlockSpec((4, ROWS, ny), lambda i, place=place: (0, place + i, 0))]
            + [vmem] * len(edges),
            out_specs=[pl.BlockSpec((groups, 4, ROWS, width), lambda i: (0, 0, i, 0))] * inner,
            scratch_shapes=[field(6), moved(2), moved(2), across, across, steps],
            cost_estimate=cost(chunk, 400),
            compiler_params=params(OUTER_MIB),
            name="outer",
        )(shear, footprint, *[volume] * 6, prev, nxt, mids[batch], *edges)
        sides = list(sides)
        for k in range(1, inner):
            pairs = [
                (g * inner + x, g * inner + (x + k) % inner)
                for g in range(groups)
                for x in range(inner)
            ]
            sides[k] = lax.ppermute(sides[k], "depth", pairs)
        received.append(sides)

    frame = None
    for number, sides in enumerate(received):
        first, step, count, _, _ = parts[number]
        chunk = count * ROWS
        pieces = pl.pallas_call(
            functools.partial(group_kernel, inner),
            out_shape=[jax.ShapeDtypeStruct((4, chunk, width), LINK)] * groups,
            in_specs=[smem] + [vmem] * inner,
            out_specs=[vmem] * groups,
            cost_estimate=pl.CostEstimate(
                flops=20 * chunk * ny, bytes_accessed=2 << 20, transcendentals=0
            ),
            compiler_params=params(16),
            name="group",
        )(shear, *sides)
        pieces = list(pieces)
        for k in range(1, groups):
            pairs = [
                (g * inner + x, (g + k) % groups * inner + x)
                for g in range(groups)
                for x in range(inner)
            ]
            pieces[k] = lax.ppermute(pieces[k], "depth", pairs)
        frame = pl.pallas_call(
            functools.partial(frame_kernel, inner, frame is not None),
            out_shape=jax.ShapeDtypeStruct((4, rows, width), jnp.float32),
            grid=(count,),
            in_specs=[smem]
            + [vmem] * groups
            + [anywhere] * (frame is not None),
            out_specs=pl.BlockSpec(
                (4, ROWS, width), lambda i, first=first, step=step: (0, first + step * i, 0)
            ),
            input_output_aliases={} if frame is None else {1 + groups: 0},
            cost_estimate=pl.CostEstimate(
                flops=20 * chunk * width, bytes_accessed=2 << 20, transcendentals=0
            ),
            compiler_params=params(16),
            name="frame",
        )(shear, *pieces, *([] if frame is None else [frame]))
    return frame


def solution(mesh):
    placed = (P("depth", "tile", None), P(), P("depth", None))
    return jax.shard_map(
        shards, mesh=mesh, in_specs=placed, out_specs=P(None, "tile", "depth"), check_vma=False
    )
```

```python
import functools

import jax
import jax.numpy as jnp
from jax import lax
from jax.experimental import pallas as pl
from jax.experimental.pallas import tpu as pltpu
from jax.sharding import PartitionSpec as P


LANES = 128
ROWS = 16
LOG2E = 1.4426950408889634
LINK = jnp.int16
INNER_MIB = 48
OUTER_MIB = 24


def params(mib):
    return pltpu.CompilerParams(vmem_limit_bytes=mib << 20)


def difference(across, steps, narrow):
    tiles = across.shape[0]
    none = jnp.zeros((ROWS, LANES), jnp.bfloat16)
    line = [none] + [narrow(t) for t in range(tiles)] + [none]
    windows = [jnp.concatenate(line[t : t + 4], axis=1) for t in range(0, tiles, 2)]
    found = jnp.dot(
        jnp.concatenate(windows, axis=0), steps[...], preferred_element_type=jnp.float32
    )
    for t in range(tiles):
        row, column = t // 2 * ROWS, t % 2 * LANES
        across[t] = found[row : row + ROWS, column : column + LANES]


def shade(field, moved_v, moved_s, across, where, shift, base, narrow):
    turn = jnp.where(shift < 0, shift + LANES, shift)
    here, up, down = pl.ds(8, ROWS), pl.ds(7, ROWS), pl.ds(9, ROWS)
    for t in range(field.shape[1]):
        dy = across[t]
        dz = field[where + 1, t, here, :] - field[where - 1, t, here, :]
        dx = field[where, t, down, :] - field[where, t, up, :]
        squares = (dx * dx + dy * dy) + (dz * dz + 4.0)
        along = (0.35 * 0.48) * dx + (0.35 * 0.6) * dy + (0.35 * 0.64) * dz
        half = 0.15 + jnp.abs(along) * lax.rsqrt(squares)
        moved_s[base, t + 1] = pltpu.roll(half, turn, 1)
        moved_v[base, t + 1] = pltpu.roll(narrow(t), turn, 1).astype(jnp.float32)


def shade_all(field, moved_v, moved_s, across, steps, count, where, shift, narrow):
    even, odd = across
    difference(even, steps, narrow(0))

    def pair_step(pair, carry):
        i = 2 * pair
        difference(odd, steps, narrow(i + 1))
        shade(field, moved_v, moved_s, even, where(i), shift(i), i, narrow(i))
        difference(even, steps, narrow(jnp.minimum(i + 2, count - 1)))
        shade(field, moved_v, moved_s, odd, where(i + 1), shift(i + 1), i + 1, narrow(i + 1))
        return carry

    lax.fori_loop(0, count // 2, pair_step, 0)


def blend(state, moved_v, moved_s, index, shift, first, count, rate):
    lane = lax.broadcasted_iota(jnp.int32, (ROWS, LANES), 1)
    turn = jnp.where(shift < 0, shift + LANES, shift)
    start = first + jnp.where(shift < 0, 1, 0)
    keep = lane < turn
    values = [moved_v[index, start + j] for j in range(count + 1)]
    shades = [moved_s[index, start + j] for j in range(count + 1)]
    result = []
    for j in range(count):
        clear, total, colours = state[j]
        v = jnp.where(keep, values[j], values[j + 1])
        half = jnp.where(keep, shades[j], shades[j + 1])
        left = clear * jnp.exp2(v * v * rate[j])
        weight = (clear - left) * half
        arguments = (0.6 * v + 0.1, -0.4 * v, 0.25 * v - 0.15)
        colours = [colours[c] + weight * jnp.tanh(arguments[c]) for c in range(3)]
        result.append((left, total + weight, colours))
    return result


def rates(absorb, footprint, first, count):
    lane = lax.broadcasted_iota(jnp.int32, (ROWS, LANES), 1)
    found = []
    for j in range(count):
        column = lane + (first + j) * LANES
        inside = (column >= footprint[0, 0]) & (column < footprint[0, 1])
        found.append(jnp.where(inside, -absorb * LOG2E, 0.0))
    return found


def fresh(count):
    zero = jnp.zeros((ROWS, LANES), jnp.float32)
    return [(zero + 1.0, zero, [zero] * 3) for _ in range(count)]


def widen(field, index, line, place):
    line = line.astype(jnp.float32)
    for t in range(field.shape[1]):
        field[index, t, place : place + line.shape[0], :] = line[:, t * LANES : (t + 1) * LANES]


def set_row(field, index, place, line):
    for t in range(field.shape[1]):
        field[index, t, place : place + 1, :] = line[:, t * LANES : (t + 1) * LANES]


def set_edges(field, slices, strip, strips, up, down, edges):
    for index, block, _ in slices:
        widen(field, index, up[block], 0)
        widen(field, index, down[block], 8 + ROWS)
    if not edges:
        return
    for edge, last, place in ((edges[0], 0, 7), (edges[1], strips - 1, 8 + ROWS)):

        @pl.when(strip == last)
        def _(edge=edge, place=place):
            line = edge[...].astype(jnp.float32)
            for index, _, s in slices:
                set_row(field, index, place, line[s : s + 1])


def prepare(moved_v, moved_s, steps):
    @pl.when(pl.program_id(0) == 0)
    def _():
        at = lax.broadcasted_iota(jnp.int32, steps.shape, 0)
        to = lax.broadcasted_iota(jnp.int32, steps.shape, 1) + LANES
        ahead = jnp.where(at == to + 1, 1.0, 0.0)
        steps[...] = jnp.where(at == to - 1, -1.0, ahead).astype(jnp.bfloat16)
        tiles = moved_v.shape[1] - 2
        zero = jnp.zeros((moved_v.shape[0], ROWS, LANES), jnp.float32)
        for t in (0, tiles + 1):
            moved_v[:, t] = zero
            moved_s[:, t] = zero


def emit(state, outs, slot, group, part, count):
    for j in range(count):
        at = pl.ds(pl.multiple_of((part * count + j) * LANES, LANES), LANES)
        clear, total, colours = state[j]
        for c in range(3):
            outs[slot][group, c, :, at] = (total + colours[c]).astype(jnp.bfloat16)
        outs[slot][group, 3, :, at] = (1.0 - clear).astype(jnp.bfloat16)


def over_columns(outs, me, inner, body):
    groups, _, _, width = outs[0].shape
    per = width // LANES
    count = min(2, per)
    for slot in range(inner):
        column = lax.rem(lax.rem(me, inner) + slot, inner)

        def column_step(i, carry, slot=slot, column=column):
            group, part = i // (per // count), lax.rem(i, per // count)
            first = (group * inner + column) * per + part * count
            emit(body(first, count), outs, slot, group, part, count)
            return carry

        lax.fori_loop(0, groups * (per // count), column_step, 0)


def inner_kernel(absorb, strip_of, strips, shear, footprint, vol, up, down, *refs):
    edges, (out, field, moved_v, moved_s, *across, steps) = refs[:-7], refs[-7:]
    slices, _, ny = vol.shape
    me = lax.axis_index("depth")
    flip = shear[0] > shear[shear.shape[0] - 1]
    prepare(moved_v, moved_s, steps)
    centre = [(s, s, s) for s in range(1, slices - 1)]
    set_edges(field, centre, strip_of(pl.program_id(0)), strips, up, down, edges)

    def widen_step(s, carry):
        widen(field, s, vol[s], 8)
        return carry

    lax.fori_loop(0, slices, widen_step, 0)

    shade_all(
        field,
        moved_v,
        moved_s,
        across,
        steps,
        slices - 2,
        lambda i: i + 1,
        lambda i: shear[me * slices + i + 1],
        lambda i: lambda t: vol[i + 1, :, t * LANES : (t + 1) * LANES],
    )

    def column_step(pair, carry):
        first = 2 * pair
        rate = rates(absorb, footprint, first, 2)
        state = fresh(2)
        for step in range(slices - 2):
            i = jnp.where(flip, slices - 3 - step, step)
            shift = shear[me * slices + i + 1]
            state = blend(state, moved_v, moved_s, i, shift, first, 2, rate)
        for j in range(2):
            at = pl.ds(pl.multiple_of((first + j) * LANES, LANES), LANES)
            clear, total, colours = state[j]
            for c in range(3):
                out[c, :, at] = total + colours[c]
            out[3, :, at] = clear
        return carry

    lax.fori_loop(0, ny // LANES // 2, column_step, 0)


def outer_kernel(absorb, inner, strip_of, strips, shear, footprint, *refs):
    front, back, front_up, front_down, back_up, back_down, prev, nxt, mid = refs[:9]
    edges, outs, (field, moved_v, moved_s, *across, steps) = refs[9 : -6 - inner], refs[-6 - inner : -6], refs[-6:]
    me = lax.axis_index("depth")
    flip = shear[0] > shear[shear.shape[0] - 1]
    slices = shear.shape[0] // lax.axis_size("depth")
    strip = strip_of(pl.program_id(0))
    prepare(moved_v, moved_s, steps)
    set_edges(field, [(1, 0, 0)], strip, strips, front_up, front_down, edges)
    set_edges(field, [(4, 0, slices - 1)], strip, strips, back_up, back_down, edges)
    for index, line in enumerate((prev, front.at[0], front.at[1], back.at[0], back.at[1], nxt)):
        widen(field, index, line[...], 8)
    ends = [front.at[0], back.at[1]]
    narrow = lambda i: lambda t: ends[i][:, t * LANES : (t + 1) * LANES]
    for i in range(2):
        difference(across[i], steps, narrow(i))
    for i in range(2):
        shift = shear[me * slices + i * (slices - 1)]
        shade(field, moved_v, moved_s, across[i], 1 + 3 * i, shift, i, narrow(i))

    def column(first, count):
        rate = rates(absorb, footprint, first, count)
        state = fresh(count)
        for step in range(2):
            i = jnp.where(flip, 1 - step, step)
            shift = shear[me * slices + i * (slices - 1)]
            state = blend(state, moved_v, moved_s, i, shift, first, count, rate)
            if step == 0:
                for j in range(count):
                    at = pl.ds(pl.multiple_of((first + j) * LANES, LANES), LANES)
                    clear, total, colours = state[j]
                    colours = [colours[c] + clear * mid[c, :, at] for c in range(3)]
                    state[j] = (clear * mid[3, :, at], total, colours)
        return state

    over_columns(outs, me, inner, column)


def encode(x):
    x = jnp.maximum(x, 1e-30)
    code = (x * lax.rsqrt(x) * 65535.0 + 0.5).astype(jnp.int32) - 32768
    return code.astype(LINK)


def decode(code):
    root = (code.astype(jnp.int32) + 32768).astype(jnp.float32) * (1.0 / 65535.0)
    return root * root


def over(pieces):
    image = pieces[0]
    for piece in pieces[1:]:
        clear = 1.0 - image[3]
        image = [image[c] + clear * piece[c] for c in range(4)]
    return image


def ordered(count, mine, flip, body):
    cases = {}
    for position in range(count):
        for turned in (False, True):
            order = tuple((position - p) % count for p in range(count))
            cases.setdefault(order[::-1] if turned else order, []).append((position, turned))
    for order, where in cases.items():
        chosen = functools.reduce(
            jnp.logical_or, [(mine == position) & (flip == turned) for position, turned in where]
        )
        pl.when(chosen)(functools.partial(body, order))


def group_kernel(inner, shear, *refs):
    groups = lax.axis_size("depth") // inner
    sources, outs = refs[:-groups], refs[-groups:]
    me = lax.axis_index("depth")
    flip = shear[0] > shear[shear.shape[0] - 1]

    def body(order):
        for part in range(len(sources) // inner):
            at = slice(part * ROWS, (part + 1) * ROWS)
            for k in range(groups):
                target = lax.rem(lax.div(me, inner) + k, groups)
                pieces = [
                    [
                        sources[part * inner + shift][target, c].astype(jnp.float32)
                        for c in range(4)
                    ]
                    for shift in order
                ]
                for c, value in enumerate(over(pieces)):
                    outs[k][c, at, :] = encode(value)

    ordered(inner, lax.rem(me, inner), flip, body)


def frame_kernel(inner, aliased, shear, *refs):
    sources, out = refs[:-1], refs[-1]
    if aliased:
        sources = sources[:-1]
    me = lax.axis_index("depth")
    flip = shear[0] > shear[shear.shape[0] - 1]

    at = pl.ds(pl.multiple_of(pl.program_id(0) * ROWS, ROWS), ROWS)

    def body(order):
        pieces = [[decode(sources[shift][c, at, :]) for c in range(4)] for shift in order]
        for c, value in enumerate(over(pieces)):
            out[c] = value

    ordered(len(sources), lax.div(me, inner), flip, body)


def shards(volume, shear, footprint):
    slices, rows, ny = volume.shape
    bricks = lax.axis_size("depth")
    crosswise = lax.axis_size("tile")
    absorb = 2.0 / (slices * bricks)
    inner = 1
    while 4 * inner * inner <= bricks:
        inner *= 2
    groups = bricks // inner
    width = ny // bricks
    tiles = ny // LANES
    strips = rows // ROWS

    def line(length):
        return [(i, i + 1) for i in range(length - 1)], [(i + 1, i) for i in range(length - 1)]

    depth_up, depth_down = line(bricks)
    row_up, row_down = line(crosswise)

    batches = [(1, strips - 2)] if strips > 2 else []
    batches += [(s, 1) for s in sorted({0, strips - 1})]
    parts = [(s, b, i) for b, (first, n) in enumerate(batches) for i, s in enumerate(range(first, first + n))]

    prev = lax.ppermute(volume[slices - 1], "depth", depth_up)
    nxt = lax.ppermute(volume[0], "depth", depth_down)
    above = lax.ppermute(volume[:, rows - 1, :], "tile", row_up)
    below = lax.ppermute(volume[:, 0, :], "tile", row_down)

    vmem = pl.BlockSpec(memory_space=pltpu.VMEM)
    smem = pl.BlockSpec(memory_space=pltpu.SMEM)
    anywhere = pl.BlockSpec(memory_space=pl.ANY)
    moved = lambda n: pltpu.VMEM((n, tiles + 2, ROWS, LANES), jnp.float32)
    field = lambda n: pltpu.VMEM((n, tiles, ROWS + 20, LANES), jnp.float32)
    across = pltpu.VMEM((tiles, ROWS, LANES), jnp.float32)
    steps = pltpu.VMEM((4 * LANES, 2 * LANES), jnp.bfloat16)

    def slab(strip_of, size, s, move=0):
        if move == 0:
            return pl.BlockSpec((size, ROWS, ny), lambda i: (s, strip_of(i), 0))
        offset = -1 if move < 0 else ROWS // 8

        def index(i):
            return s, jnp.clip(strip_of(i) * (ROWS // 8) + offset, 0, rows // 8 - 1), 0

        return pl.BlockSpec((size, 8, ny), index)

    def cost(chunk, per):
        return pl.CostEstimate(
            flops=per * chunk * ny, bytes_accessed=chunk * ny * 32, transcendentals=0
        )

    mids = []
    for first, count in batches:
        strip_of = lambda i, first=first: first + i
        edges = [above, below] if first == 0 or first + count == strips else []
        mid = pl.pallas_call(
            functools.partial(inner_kernel, absorb, strip_of, strips),
            out_shape=jax.ShapeDtypeStruct((4, count * ROWS, ny), jnp.float32),
            grid=(count,),
            in_specs=[smem, smem]
            + [slab(strip_of, slices, 0, move) for move in (0, -1, 1)]
            + [vmem] * len(edges),
            out_specs=pl.BlockSpec((4, ROWS, ny), lambda i: (0, i, 0)),
            scratch_shapes=[field(slices), moved(slices - 2), moved(slices - 2)]
            + [across, across, steps],
            cost_estimate=cost(count * ROWS, 800),
            compiler_params=params(INNER_MIB),
            name="inner",
        )(shear, footprint, *[volume] * 3, *edges)
        mids.append(mid)

    received = []
    count, chunk = 1, ROWS
    for first, batch, place in parts:
        strip_of = lambda i, first=first: first + i
        edges = [above, below] if first in (0, strips - 1) else []
        flat = pl.BlockSpec((ROWS, ny), lambda i, first=first: (first + i, 0))
        ends = [(2, 0, 0), (2, slices // 2 - 1, 0)]
        ends += [(1, s, move) for s in (0, slices - 1) for move in (-1, 1)]
        sides = pl.pallas_call(
            functools.partial(outer_kernel, absorb, inner, strip_of, strips),
            out_shape=[jax.ShapeDtypeStruct((groups, 4, chunk, width), jnp.bfloat16)] * inner,
            grid=(count,),
            in_specs=[smem, smem]
            + [slab(strip_of, *end) for end in ends]
            + [flat, flat]
            + [pl.BlockSpec((4, ROWS, ny), lambda i, place=place: (0, place + i, 0))]
            + [vmem] * len(edges),
            out_specs=[pl.BlockSpec((groups, 4, ROWS, width), lambda i: (0, 0, i, 0))] * inner,
            scratch_shapes=[field(6), moved(2), moved(2), across, across, steps],
            cost_estimate=cost(chunk, 400),
            compiler_params=params(OUTER_MIB),
            name="outer",
        )(shear, footprint, *[volume] * 6, prev, nxt, mids[batch], *edges)
        sides = list(sides)
        for k in range(1, inner):
            pairs = [
                (g * inner + x, g * inner + (x + k) % inner)
                for g in range(groups)
                for x in range(inner)
            ]
            sides[k] = lax.ppermute(sides[k], "depth", pairs)
        received.append(sides)

    frame = None
    middle = max(strips - 2, 0)
    stages = ([range(middle)] if middle else []) + [[n] for n in range(middle, len(parts))]
    for stage in stages:
        first, count = parts[stage[0]][0], len(stage)
        chunk = count * ROWS
        sides = [side for n in stage for side in received[n]]
        pieces = pl.pallas_call(
            functools.partial(group_kernel, inner),
            out_shape=[jax.ShapeDtypeStruct((4, chunk, width), LINK)] * groups,
            in_specs=[smem] + [vmem] * len(sides),
            out_specs=[vmem] * groups,
            cost_estimate=pl.CostEstimate(
                flops=20 * chunk * ny, bytes_accessed=2 << 20, transcendentals=0
            ),
            compiler_params=params(16),
            name="group",
        )(shear, *sides)
        pieces = list(pieces)
        for k in range(1, groups):
            pairs = [
                (g * inner + x, (g + k) % groups * inner + x)
                for g in range(groups)
                for x in range(inner)
            ]
            pieces[k] = lax.ppermute(pieces[k], "depth", pairs)
        frame = pl.pallas_call(
            functools.partial(frame_kernel, inner, frame is not None),
            out_shape=jax.ShapeDtypeStruct((4, rows, width), jnp.float32),
            grid=(count,),
            in_specs=[smem]
            + [vmem] * groups
            + [anywhere] * (frame is not None),
            out_specs=pl.BlockSpec(
                (4, ROWS, width), lambda i, first=first: (0, first + i, 0)
            ),
            input_output_aliases={} if frame is None else {1 + groups: 0},
            cost_estimate=pl.CostEstimate(
                flops=20 * chunk * width, bytes_accessed=2 << 20, transcendentals=0
            ),
            compiler_params=params(16),
            name="frame",
        )(shear, *pieces, *([] if frame is None else [frame]))
    return frame


def solution(mesh):
    placed = (P("depth", "tile", None), P(), P("depth", None))
    return jax.shard_map(
        shards, mesh=mesh, in_specs=placed, out_specs=P(None, "tile", "depth"), check_vma=False
    )
```

```python
import functools

import jax
import jax.numpy as jnp
from jax import lax
from jax.experimental import pallas as pl
from jax.experimental.pallas import tpu as pltpu
from jax.sharding import PartitionSpec as P


LANES = 128
ROWS = 16
LOG2E = 1.4426950408889634
LINK = jnp.int16
INNER_MIB = 48
OUTER_MIB = 24


def params(mib):
    return pltpu.CompilerParams(vmem_limit_bytes=mib << 20)


def difference(across, steps, narrow):
    tiles = across.shape[0]
    none = jnp.zeros((ROWS, LANES), jnp.bfloat16)
    line = [none] + [narrow(t) for t in range(tiles)] + [none]
    windows = [jnp.concatenate(line[t : t + 4], axis=1) for t in range(0, tiles, 2)]
    found = jnp.dot(
        jnp.concatenate(windows, axis=0), steps[...], preferred_element_type=jnp.float32
    )
    for t in range(tiles):
        row, column = t // 2 * ROWS, t % 2 * LANES
        across[t] = found[row : row + ROWS, column : column + LANES]


def shade(field, moved_v, moved_s, across, where, shift, base, narrow):
    turn = jnp.where(shift < 0, shift + LANES, shift)
    here, up, down = pl.ds(8, ROWS), pl.ds(7, ROWS), pl.ds(9, ROWS)
    for t in range(field.shape[1]):
        dy = across[t]
        dz = field[where + 1, t, here, :] - field[where - 1, t, here, :]
        dx = field[where, t, down, :] - field[where, t, up, :]
        squares = (dx * dx + dy * dy) + (dz * dz + 4.0)
        along = (0.35 * 0.48) * dx + (0.35 * 0.6) * dy + (0.35 * 0.64) * dz
        half = 0.15 + jnp.abs(along) * lax.rsqrt(squares)
        moved_s[base, t + 1] = pltpu.roll(half, turn, 1)
        moved_v[base, t + 1] = pltpu.roll(narrow(t), turn, 1).astype(jnp.float32)


def shade_all(field, moved_v, moved_s, across, steps, count, where, shift, narrow):
    even, odd = across
    difference(even, steps, narrow(0))

    def pair_step(pair, carry):
        i = 2 * pair
        difference(odd, steps, narrow(i + 1))
        shade(field, moved_v, moved_s, even, where(i), shift(i), i, narrow(i))
        difference(even, steps, narrow(jnp.minimum(i + 2, count - 1)))
        shade(field, moved_v, moved_s, odd, where(i + 1), shift(i + 1), i + 1, narrow(i + 1))
        return carry

    lax.fori_loop(0, count // 2, pair_step, 0)


def blend(state, moved_v, moved_s, index, shift, first, count, rate):
    lane = lax.broadcasted_iota(jnp.int32, (ROWS, LANES), 1)
    turn = jnp.where(shift < 0, shift + LANES, shift)
    start = first + jnp.where(shift < 0, 1, 0)
    keep = lane < turn
    values = [moved_v[index, start + j] for j in range(count + 1)]
    shades = [moved_s[index, start + j] for j in range(count + 1)]
    result = []
    for j in range(count):
        clear, total, colours = state[j]
        v = jnp.where(keep, values[j], values[j + 1])
        half = jnp.where(keep, shades[j], shades[j + 1])
        left = clear * jnp.exp2(v * v * rate[j])
        weight = (clear - left) * half
        arguments = (0.6 * v + 0.1, -0.4 * v, 0.25 * v - 0.15)
        colours = [colours[c] + weight * jnp.tanh(arguments[c]) for c in range(3)]
        result.append((left, total + weight, colours))
    return result


def rates(absorb, footprint, first, count):
    lane = lax.broadcasted_iota(jnp.int32, (ROWS, LANES), 1)
    found = []
    for j in range(count):
        column = lane + (first + j) * LANES
        inside = (column >= footprint[0, 0]) & (column < footprint[0, 1])
        found.append(jnp.where(inside, -absorb * LOG2E, 0.0))
    return found


def fresh(count):
    zero = jnp.zeros((ROWS, LANES), jnp.float32)
    return [(zero + 1.0, zero, [zero] * 3) for _ in range(count)]


def widen(field, index, line, place):
    line = line.astype(jnp.float32)
    for t in range(field.shape[1]):
        field[index, t, place : place + line.shape[0], :] = line[:, t * LANES : (t + 1) * LANES]


def set_row(field, index, place, line):
    for t in range(field.shape[1]):
        field[index, t, place : place + 1, :] = line[:, t * LANES : (t + 1) * LANES]


def set_edges(field, slices, strip, strips, up, down, edges):
    for index, block, _ in slices:
        widen(field, index, up[block], 0)
        widen(field, index, down[block], 8 + ROWS)
    if not edges:
        return
    for edge, last, place in ((edges[0], 0, 7), (edges[1], strips - 1, 8 + ROWS)):

        @pl.when(strip == last)
        def _(edge=edge, place=place):
            line = edge[...].astype(jnp.float32)
            for index, _, s in slices:
                set_row(field, index, place, line[s : s + 1])


def prepare(moved_v, moved_s, steps):
    @pl.when(pl.program_id(0) == 0)
    def _():
        at = lax.broadcasted_iota(jnp.int32, steps.shape, 0)
        to = lax.broadcasted_iota(jnp.int32, steps.shape, 1) + LANES
        ahead = jnp.where(at == to + 1, 1.0, 0.0)
        steps[...] = jnp.where(at == to - 1, -1.0, ahead).astype(jnp.bfloat16)
        tiles = moved_v.shape[1] - 2
        zero = jnp.zeros((moved_v.shape[0], ROWS, LANES), jnp.float32)
        for t in (0, tiles + 1):
            moved_v[:, t] = zero
            moved_s[:, t] = zero


def emit(state, outs, slot, group, part, count):
    for j in range(count):
        at = pl.ds(pl.multiple_of((part * count + j) * LANES, LANES), LANES)
        clear, total, colours = state[j]
        for c in range(3):
            outs[slot][group, c, :, at] = (total + colours[c]).astype(jnp.bfloat16)
        outs[slot][group, 3, :, at] = (1.0 - clear).astype(jnp.bfloat16)


def over_columns(outs, me, inner, body):
    groups, _, _, width = outs[0].shape
    per = width // LANES
    count = min(4, per)
    for slot in range(inner):
        column = lax.rem(lax.rem(me, inner) + slot, inner)

        def column_step(i, carry, slot=slot, column=column):
            group, part = i // (per // count), lax.rem(i, per // count)
            first = (group * inner + column) * per + part * count
            emit(body(first, count), outs, slot, group, part, count)
            return carry

        lax.fori_loop(0, groups * (per // count), column_step, 0)


def inner_kernel(absorb, strip_of, strips, shear, footprint, vol, up, down, *refs):
    edges, (out, field, moved_v, moved_s, *across, steps) = refs[:-7], refs[-7:]
    slices, _, ny = vol.shape
    me = lax.axis_index("depth")
    flip = shear[0] > shear[shear.shape[0] - 1]
    prepare(moved_v, moved_s, steps)
    centre = [(s, s, s) for s in range(1, slices - 1)]
    set_edges(field, centre, strip_of(pl.program_id(0)), strips, up, down, edges)

    def widen_step(s, carry):
        widen(field, s, vol[s], 8)
        return carry

    lax.fori_loop(0, slices, widen_step, 0)

    shade_all(
        field,
        moved_v,
        moved_s,
        across,
        steps,
        slices - 2,
        lambda i: i + 1,
        lambda i: shear[me * slices + i + 1],
        lambda i: lambda t: vol[i + 1, :, t * LANES : (t + 1) * LANES],
    )

    def column_step(pair, carry):
        first = 2 * pair
        rate = rates(absorb, footprint, first, 2)
        state = fresh(2)
        for step in range(slices - 2):
            i = jnp.where(flip, slices - 3 - step, step)
            shift = shear[me * slices + i + 1]
            state = blend(state, moved_v, moved_s, i, shift, first, 2, rate)
        for j in range(2):
            at = pl.ds(pl.multiple_of((first + j) * LANES, LANES), LANES)
            clear, total, colours = state[j]
            for c in range(3):
                out[c, :, at] = total + colours[c]
            out[3, :, at] = clear
        return carry

    lax.fori_loop(0, ny // LANES // 2, column_step, 0)


def outer_kernel(absorb, inner, strip_of, strips, shear, footprint, *refs):
    front, back, front_up, front_down, back_up, back_down, prev, nxt, mid = refs[:9]
    edges, outs, (field, moved_v, moved_s, *across, steps) = refs[9 : -6 - inner], refs[-6 - inner : -6], refs[-6:]
    me = lax.axis_index("depth")
    flip = shear[0] > shear[shear.shape[0] - 1]
    slices = shear.shape[0] // lax.axis_size("depth")
    strip = strip_of(pl.program_id(0))
    prepare(moved_v, moved_s, steps)
    set_edges(field, [(1, 0, 0)], strip, strips, front_up, front_down, edges)
    set_edges(field, [(4, 0, slices - 1)], strip, strips, back_up, back_down, edges)
    for index, line in enumerate((prev, front.at[0], front.at[1], back.at[0], back.at[1], nxt)):
        widen(field, index, line[...], 8)
    ends = [front.at[0], back.at[1]]
    narrow = lambda i: lambda t: ends[i][:, t * LANES : (t + 1) * LANES]
    for i in range(2):
        difference(across[i], steps, narrow(i))
    for i in range(2):
        shift = shear[me * slices + i * (slices - 1)]
        shade(field, moved_v, moved_s, across[i], 1 + 3 * i, shift, i, narrow(i))

    def column(first, count):
        rate = rates(absorb, footprint, first, count)
        state = fresh(count)
        for step in range(2):
            i = jnp.where(flip, 1 - step, step)
            shift = shear[me * slices + i * (slices - 1)]
            state = blend(state, moved_v, moved_s, i, shift, first, count, rate)
            if step == 0:
                for j in range(count):
                    at = pl.ds(pl.multiple_of((first + j) * LANES, LANES), LANES)
                    clear, total, colours = state[j]
                    colours = [colours[c] + clear * mid[c, :, at] for c in range(3)]
                    state[j] = (clear * mid[3, :, at], total, colours)
        return state

    over_columns(outs, me, inner, column)


def encode(x):
    x = jnp.maximum(x, 1e-30)
    code = (x * lax.rsqrt(x) * 65535.0 + 0.5).astype(jnp.int32) - 32768
    return code.astype(LINK)


def decode(code):
    root = (code.astype(jnp.int32) + 32768).astype(jnp.float32) * (1.0 / 65535.0)
    return root * root


def over(pieces):
    image = pieces[0]
    for piece in pieces[1:]:
        clear = 1.0 - image[3]
        image = [image[c] + clear * piece[c] for c in range(4)]
    return image


def ordered(count, mine, flip, body):
    cases = {}
    for position in range(count):
        for turned in (False, True):
            order = tuple((position - p) % count for p in range(count))
            cases.setdefault(order[::-1] if turned else order, []).append((position, turned))
    for order, where in cases.items():
        chosen = functools.reduce(
            jnp.logical_or, [(mine == position) & (flip == turned) for position, turned in where]
        )
        pl.when(chosen)(functools.partial(body, order))


def group_kernel(inner, shear, *refs):
    sources, outs = refs[:inner], refs[inner:]
    me = lax.axis_index("depth")
    flip = shear[0] > shear[shear.shape[0] - 1]
    groups = len(outs)

    def body(order):
        def step(i, carry):
            at = pl.ds(pl.multiple_of(i * ROWS, ROWS), ROWS)
            for k in range(groups):
                target = lax.rem(lax.div(me, inner) + k, groups)
                pieces = [
                    [sources[shift][target, c, at, :].astype(jnp.float32) for c in range(4)]
                    for shift in order
                ]
                for c, value in enumerate(over(pieces)):
                    outs[k][c, at, :] = encode(value)
            return carry

        lax.fori_loop(0, outs[0].shape[1] // ROWS, step, 0)

    ordered(inner, lax.rem(me, inner), flip, body)


def frame_kernel(inner, aliased, shear, *refs):
    sources, out = refs[:-1], refs[-1]
    if aliased:
        sources = sources[:-1]
    me = lax.axis_index("depth")
    flip = shear[0] > shear[shear.shape[0] - 1]

    at = pl.ds(pl.multiple_of(pl.program_id(0) * ROWS, ROWS), ROWS)

    def body(order):
        pieces = [[decode(sources[shift][c, at, :]) for c in range(4)] for shift in order]
        for c, value in enumerate(over(pieces)):
            out[c] = value

    ordered(len(sources), lax.div(me, inner), flip, body)


def shards(volume, shear, footprint):
    slices, rows, ny = volume.shape
    bricks = lax.axis_size("depth")
    crosswise = lax.axis_size("tile")
    absorb = 2.0 / (slices * bricks)
    inner = 1
    while 4 * inner * inner <= bricks:
        inner *= 2
    groups = bricks // inner
    width = ny // bricks
    tiles = ny // LANES
    strips = rows // ROWS

    def line(length):
        return [(i, i + 1) for i in range(length - 1)], [(i + 1, i) for i in range(length - 1)]

    depth_up, depth_down = line(bricks)
    row_up, row_down = line(crosswise)

    batches = [(1, strips - 2)] if strips > 2 else []
    batches += [(s, 1) for s in sorted({0, strips - 1})]
    parts = [(s, b, i) for b, (first, n) in enumerate(batches) for i, s in enumerate(range(first, first + n))]

    prev = lax.ppermute(volume[slices - 1], "depth", depth_up)
    nxt = lax.ppermute(volume[0], "depth", depth_down)
    above = lax.ppermute(volume[:, rows - 1, :], "tile", row_up)
    below = lax.ppermute(volume[:, 0, :], "tile", row_down)

    vmem = pl.BlockSpec(memory_space=pltpu.VMEM)
    smem = pl.BlockSpec(memory_space=pltpu.SMEM)
    anywhere = pl.BlockSpec(memory_space=pl.ANY)
    moved = lambda n: pltpu.VMEM((n, tiles + 2, ROWS, LANES), jnp.float32)
    field = lambda n: pltpu.VMEM((n, tiles, ROWS + 20, LANES), jnp.float32)
    across = pltpu.VMEM((tiles, ROWS, LANES), jnp.float32)
    steps = pltpu.VMEM((4 * LANES, 2 * LANES), jnp.bfloat16)

    def slab(strip_of, size, s, move=0):
        if move == 0:
            return pl.BlockSpec((size, ROWS, ny), lambda i: (s, strip_of(i), 0))
        offset = -1 if move < 0 else ROWS // 8

        def index(i):
            return s, jnp.clip(strip_of(i) * (ROWS // 8) + offset, 0, rows // 8 - 1), 0

        return pl.BlockSpec((size, 8, ny), index)

    def cost(chunk, per):
        return pl.CostEstimate(
            flops=per * chunk * ny, bytes_accessed=chunk * ny * 32, transcendentals=0
        )

    mids = []
    for first, count in batches:
        strip_of = lambda i, first=first: first + i
        edges = [above, below] if first == 0 or first + count == strips else []
        mid = pl.pallas_call(
            functools.partial(inner_kernel, absorb, strip_of, strips),
            out_shape=jax.ShapeDtypeStruct((4, count * ROWS, ny), jnp.float32),
            grid=(count,),
            in_specs=[smem, smem]
            + [slab(strip_of, slices, 0, move) for move in (0, -1, 1)]
            + [vmem] * len(edges),
            out_specs=pl.BlockSpec((4, ROWS, ny), lambda i: (0, i, 0)),
            scratch_shapes=[field(slices), moved(slices - 2), moved(slices - 2)]
            + [across, across, steps],
            cost_estimate=cost(count * ROWS, 800),
            compiler_params=params(INNER_MIB),
            name="inner",
        )(shear, footprint, *[volume] * 3, *edges)
        mids.append(mid)

    received = []
    count, chunk = 1, ROWS
    for first, batch, place in parts:
        strip_of = lambda i, first=first: first + i
        edges = [above, below] if first in (0, strips - 1) else []
        flat = pl.BlockSpec((ROWS, ny), lambda i, first=first: (first + i, 0))
        ends = [(2, 0, 0), (2, slices // 2 - 1, 0)]
        ends += [(1, s, move) for s in (0, slices - 1) for move in (-1, 1)]
        sides = pl.pallas_call(
            functools.partial(outer_kernel, absorb, inner, strip_of, strips),
            out_shape=[jax.ShapeDtypeStruct((groups, 4, chunk, width), jnp.bfloat16)] * inner,
            grid=(count,),
            in_specs=[smem, smem]
            + [slab(strip_of, *end) for end in ends]
            + [flat, flat]
            + [pl.BlockSpec((4, ROWS, ny), lambda i, place=place: (0, place + i, 0))]
            + [vmem] * len(edges),
            out_specs=[pl.BlockSpec((groups, 4, ROWS, width), lambda i: (0, 0, i, 0))] * inner,
            scratch_shapes=[field(6), moved(2), moved(2), across, across, steps],
            cost_estimate=cost(chunk, 400),
            compiler_params=params(OUTER_MIB),
            name="outer",
        )(shear, footprint, *[volume] * 6, prev, nxt, mids[batch], *edges)
        sides = list(sides)
        for k in range(1, inner):
            pairs = [
                (g * inner + x, g * inner + (x + k) % inner)
                for g in range(groups)
                for x in range(inner)
            ]
            sides[k] = lax.ppermute(sides[k], "depth", pairs)
        received.append(sides)

    frame = None
    for number, sides in enumerate(received):
        first = parts[number][0]
        pieces = pl.pallas_call(
            functools.partial(group_kernel, inner),
            out_shape=[jax.ShapeDtypeStruct((4, chunk, width), LINK)] * groups,
            in_specs=[smem] + [vmem] * inner,
            out_specs=[vmem] * groups,
            cost_estimate=pl.CostEstimate(
                flops=20 * chunk * ny, bytes_accessed=2 << 20, transcendentals=0
            ),
            compiler_params=params(16),
            name="group",
        )(shear, *sides)
        pieces = list(pieces)
        for k in range(1, groups):
            pairs = [
                (g * inner + x, (g + k) % groups * inner + x)
                for g in range(groups)
                for x in range(inner)
            ]
            pieces[k] = lax.ppermute(pieces[k], "depth", pairs)
        frame = pl.pallas_call(
            functools.partial(frame_kernel, inner, frame is not None),
            out_shape=jax.ShapeDtypeStruct((4, rows, width), jnp.float32),
            grid=(count,),
            in_specs=[smem]
            + [vmem] * groups
            + [anywhere] * (frame is not None),
            out_specs=pl.BlockSpec(
                (4, ROWS, width), lambda i, first=first: (0, first + i, 0)
            ),
            input_output_aliases={} if frame is None else {1 + groups: 0},
            cost_estimate=pl.CostEstimate(
                flops=20 * chunk * width, bytes_accessed=2 << 20, transcendentals=0
            ),
            compiler_params=params(16),
            name="frame",
        )(shear, *pieces, *([] if frame is None else [frame]))
    return frame


def solution(mesh):
    placed = (P("depth", "tile", None), P(), P("depth", None))
    return jax.shard_map(
        shards, mesh=mesh, in_specs=placed, out_specs=P(None, "tile", "depth"), check_vma=False
    )
```
